128 devices in a mesh: rep: 1, dp: 128 (over x, y, z, core).
Axes of the slice: x: 4, y: 4, z: 4, core: 2. Of those that a mesh axis runs over, the one named last changes fastest.
Arguments:
- g_w_gate: bfloat16 [128, 2, 512, 8192], P(('rep', 'dp'))
- g_w_up: bfloat16 [128, 2, 512, 8192], P(('rep', 'dp'))
- g_w_down: bfloat16 [128, 2, 8192, 512], P(('rep', 'dp'))
- w_gate: bfloat16 [2, 512, 8192], replicated
- w_up: bfloat16 [2, 512, 8192], replicated
- w_down: bfloat16 [2, 8192, 512], replicated
- m_w_gate: float32 [2, 512, 8192], P(None, 'dp')
- m_w_up: float32 [2, 512, 8192], P(None, 'dp')
- m_w_down: float32 [2, 8192, 512], P(None, 'dp')
- v_w_gate: float32 [2, 512, 8192], P(None, 'dp')
- v_w_up: float32 [2, 512, 8192], P(None, 'dp')
- v_w_down: float32 [2, 8192, 512], P(None, 'dp')
Outputs:
- output 1: bfloat16 [2, 512, 8192], P('rep')
- output 2: bfloat16 [2, 512, 8192], P('rep')
- output 3: bfloat16 [2, 8192, 512], P('rep')
- output 4: float32 [2, 512, 8192], P('rep', 'dp')
- output 5: float32 [2, 512, 8192], P('rep', 'dp')
- output 6: float32 [2, 8192, 512], P('rep', 'dp')
- output 7: float32 [2, 512, 8192], P('rep', 'dp')
- output 8: float32 [2, 512, 8192], P('rep', 'dp')
- output 9: float32 [2, 8192, 512], P('rep', 'dp')
All inputs are finite; a program needn't handle non-finite values.
Results may differ from the reference program's by a relative error of at most 0.022.
Values are sent between devices in bfloat16 or wider.
A program may use at most 1.5 GiB of HBM per device.

```python
import jax
import jax.numpy as jnp
from jax import lax

DEVICES = 128
D = 512
FF = 8192
LAYERS = 2
NAMES = ("w_gate", "w_up", "w_down")
SHAPES = {"w_gate": (LAYERS, D, FF), "w_up": (LAYERS, D, FF), "w_down": (LAYERS, FF, D)}


def setup_inputs(seed: int = 0, part: int = 0) -> dict:
    kz, *keys = jax.random.split(jax.random.key(seed), 1 + 5 * len(NAMES))
    loud = 2.0 ** jax.random.uniform(kz, (), jnp.float32, -1.0, 1.0)
    drawn = {}
    for name, key, both in zip(NAMES, keys[:3], keys[3:6], strict=True):
        own = jax.random.normal(jax.random.fold_in(key, part), (DEVICES, *SHAPES[name]), jnp.float32)
        shared = jax.random.normal(jax.random.fold_in(both, part), SHAPES[name], jnp.float32)
        drawn["g_" + name] = (loud * (0.7 * shared / DEVICES + 0.7 * own * DEVICES**-0.5)).astype(jnp.bfloat16)
    for name, key in zip(NAMES, keys[6:9], strict=True):
        drawn[name] = (jax.random.normal(key, SHAPES[name], jnp.float32) * SHAPES[name][1] ** -0.5).astype(jnp.bfloat16)
    for name, key in zip(NAMES, keys[9:12], strict=True):
        drawn["m_" + name] = loud * 0.5 * jax.random.normal(key, SHAPES[name], jnp.float32)
    for name, key in zip(NAMES, keys[12:15], strict=True):
        drawn["v_" + name] = loud * loud * jax.random.uniform(key, SHAPES[name], jnp.float32, 0.5, 1.5)
    return drawn


def adamw(w, m, v, g):
    m = 0.9 * m + 0.1 * g
    v = 0.95 * v + 0.05 * g * g
    step = m * lax.rsqrt(v + 1e-8) + 0.1 * w
    return (w - 0.02 * step).astype(jnp.bfloat16), m, v


def reference(g_w_gate, g_w_up, g_w_down, w_gate, w_up, w_down, m_w_gate, m_w_up, m_w_down, v_w_gate, v_w_up, v_w_down):
    def total(terms):
        return lax.scan(lambda so_far, term: (so_far + term.astype(jnp.float32), None), jnp.zeros(terms.shape[1:], jnp.float32), terms)[0]

    gradients = [total(terms).astype(jnp.bfloat16).astype(jnp.float32) for terms in (g_w_gate, g_w_up, g_w_down)]
    new = [
        adamw(w.astype(jnp.float32), m, v, g)
        for w, m, v, g in zip((w_gate, w_up, w_down), (m_w_gate, m_w_up, m_w_down), (v_w_gate, v_w_up, v_w_down), gradients, strict=True)
    ]
    return tuple(one[which] for which in range(3) for one in new)
```

```python
import functools

import jax
import jax.numpy as jnp
from jax import lax
from jax.experimental import pallas as pl
from jax.experimental.pallas import tpu as pltpu
from jax.sharding import PartitionSpec as P

N = 4
MESH = pl.DeviceIdType.MESH
ORDER = ((0, 1, 2), (1, 2, 0), (2, 0, 1))
SIDES = (1, -1)
WEIGHTS = range(3)


def adamw(w, m, v, g):
    m = 0.9 * m + 0.1 * g
    v = 0.95 * v + 0.05 * g * g
    step = m * lax.rsqrt(v + 1e-8) + 0.1 * w
    return w - 0.02 * step, m, v


def place():
    me = lax.axis_index("dp")
    core = lax.rem(me, 2)
    chip = me // 2
    return (chip // (N * N), lax.rem(chip // N, N), lax.rem(chip, N)), core


def device(chip, core):
    return {"dp": ((chip[0] * N + chip[1]) * N + chip[2]) * 2 + core}


def neighbour(chip, core, axis, side):
    moved = list(chip)
    moved[axis] = lax.rem(chip[axis] + side + N, N)
    return device(moved, core)


def greet(chip, core):
    barrier = pltpu.get_barrier_semaphore()
    others = [device(chip, 1 - core)] + [neighbour(chip, core, axis, side) for axis in range(3) for side in SIDES]
    for other in others:
        pl.semaphore_signal(barrier, inc=1, device_id=other, device_id_type=MESH)
    pl.semaphore_wait(barrier, len(others))


def piece(ref, k, layer, i1, i2, h):
    if k == 2:
        return ref.at[layer, i2, :, i1, h]
    half = ref.shape[-1] // 2
    columns = pl.ds(pl.multiple_of(h * half, half), half)
    if k == 0:
        return ref.at[layer, i1, i2, :, :, columns]
    return ref.at[layer, :, i1, i2, :, columns]


def far(m):
    return (4 - m) // 2


def half_of(side, m):
    h = lax.rem(m, 2) * (1 - m // 2) if not isinstance(m, int) else (m % 2) * (1 - m // 2)
    return h if side == 1 else 1 - h


def target(mine, side, m):
    return lax.rem(mine + side * far(m) + N, N)


def turn(mine, s):
    return lax.rem(mine + 2 - s + (s // 2) * (2 * s - 1) + N, N)


def put_sum(out, sources):
    def one(out, sources):
        total = sources[0][...].astype(jnp.float32)
        for source in sources[1:]:
            total = total + source[...].astype(jnp.float32)
        out[...] = total.astype(out.dtype)

    if len(out.shape) == 2:
        one(out, sources)
    else:

        @pl.loop(0, out.shape[0])
        def _(i):
            one(out.at[i], [source.at[i] for source in sources])


def scatter_kernel(*refs):
    g, out = refs[0:3], refs[3:6]
    part, r1, r2, r3, ahead, kept = (refs[6 + 3 * i : 9 + 3 * i] for i in range(6))
    part_in, part_out, in1, out1, in2, out2, in3, out3, ahead_in, kept_in, swap_in, swap_out = refs[24:]
    chip, core = place()
    partner = device(chip, 1 - core)
    at = [[chip[axis] for axis in ORDER[k]] for k in WEIGHTS]
    lanes = [(k, d, side) for d, side in enumerate(SIDES) for k in WEIGHTS]
    greet(chip, core)

    def split(t):
        return t // N, lax.rem(t, N)

    def spot(k, side, t):
        m, s = split(t)
        return target(at[k][0], side, m), turn(at[k][1], s), half_of(side, m)

    def give(t):
        for k, d, side in lanes:
            i1, i2, h = spot(k, side, t)
            pltpu.make_async_remote_copy(
                src_ref=piece(g[k], k, 1 - core, i1, i2, h),
                dst_ref=part[k].at[i1, i2, h],
                send_sem=part_out.at[k],
                recv_sem=part_in.at[k, i1, i2, h],
                device_id=partner,
                device_id_type=MESH,
            ).start()

    def fetch(t):
        for k, d, side in lanes:
            i1, i2, h = spot(k, side, t)
            slot = lax.rem(t, 2)
            yield pltpu.make_async_copy(piece(g[k], k, core, i1, i2, h), ahead[k].at[slot, d], ahead_in.at[k, slot, d])

    def part_arrived(k, i1, i2, h):
        ref = part[k].at[i1, i2, h]
        pltpu.make_async_copy(ref, ref, part_in.at[k, i1, i2, h]).wait()

    def arrived(ref, sem):
        pltpu.make_async_copy(ref, ref, sem).wait()

    def send(k, axis, side, src, dst, out_sem, in_sem):
        pltpu.make_async_remote_copy(
            src_ref=src, dst_ref=dst, send_sem=out_sem, recv_sem=in_sem,
            device_id=neighbour(chip, core, ORDER[k][axis], side), device_id_type=MESH,
        ).start()

    @pl.loop(0, N)
    def _(t):
        give(t)

    for copy in fetch(0):
        copy.start()

    def own_copies():
        for k in WEIGHTS:
            for i2 in range(N):
                for h in range(2):
                    yield pltpu.make_async_copy(piece(g[k], k, core, at[k][0], i2, h), kept[k].at[i2, h], kept_in.at[k])

    def first(last):
        def body(t):
            give(t + N)
            if last:

                @pl.when(t + 1 < 3 * N)
                def _():
                    for copy in fetch(t + 1):
                        copy.start()
            else:
                for copy in fetch(t + 1):
                    copy.start()
            pending = None
            for (k, d, side), copy in zip(lanes, fetch(t), strict=True):
                i1, i2, h = spot(k, side, t)
                copy.wait()
                part_arrived(k, i1, i2, h)
                here = part[k].at[i1, i2, h]
                sources = [here, ahead[k].at[lax.rem(t, 2), d]]
                if last:
                    arrived(r1[k].at[d, 0, i2], in1.at[k, d, 0, i2])
                    sources.append(r1[k].at[d, 0, i2])
                put_sum(here, sources)
                if pending is not None:
                    pending()
                m = 2 if last else t // N
                pending = functools.partial(send, k, 0, side, here, r1[k].at[d, m, i2], out1.at[k, d], in1.at[k, d, m, i2])
            pending()

        return body

    pl.loop(0, 2 * N)(first(False))
    for copy in own_copies():
        copy.start()
    pl.loop(2 * N, 3 * N)(first(True))

    for k in WEIGHTS:
        pltpu.make_async_copy(kept[k], kept[k], kept_in.at[k]).wait()

    def settled(k, side, m):
        i2, h = target(at[k][1], side, m), half_of(side, m)
        part_arrived(k, at[k][0], i2, h)
        for d, m1 in ((0, 2 - h), (1, 1 + h)):
            arrived(r1[k].at[d, m1, i2], in1.at[k, d, m1, i2])

    def terms1(k, i2, h, i3):
        here = part[k].at[at[k][0], i2, h, i3]
        return here, [here, kept[k].at[i2, h, i3], r1[k].at[0, 2 - h, i2, i3], r1[k].at[1, 1 + h, i2, i3]]

    for m in range(3):
        for k, d, side in lanes:
            settled(k, side, m)

        @pl.loop(0, N)
        def _(s):
            pending = None
            for k, d, side in lanes:
                i2, h, i3 = target(at[k][1], side, m), half_of(side, m), turn(at[k][2], s)
                here, sources = terms1(k, i2, h, i3)
                if m == 2:
                    arrived(r2[k].at[d, 0, i3], in2.at[k, d, 0, i3])
                    sources.append(r2[k].at[d, 0, i3])
                put_sum(here, sources)
                if pending is not None:
                    pending()
                pending = functools.partial(send, k, 1, side, here, r2[k].at[d, m, i3], out2.at[k, d], in2.at[k, d, m, i3])
            pending()

    for k, d, side in lanes:
        settled(k, side, 3)
    for m in range(4):
        pending = None
        for k, d, side in lanes:
            i2, h, i3 = at[k][1], half_of(side, m), target(at[k][2], side, m)
            here, sources = terms1(k, i2, h, i3)
            for e, m2 in ((0, 2 - h), (1, 1 + h)):
                arrived(r2[k].at[e, m2, i3], in2.at[k, e, m2, i3])
                sources.append(r2[k].at[e, m2, i3])
            if m == 2:
                arrived(r3[k].at[d, 0], in3.at[k, d, 0])
                sources.append(r3[k].at[d, 0])
            if m == 3:
                for e, m3 in ((0, 2 - h), (1, 1 + h)):
                    arrived(r3[k].at[e, m3], in3.at[k, e, m3])
                    sources.append(r3[k].at[e, m3])
                here = out[k].at[core, h]
            put_sum(here, sources)
            if pending is not None:
                pending()
            pending = None
            if m < 3:
                pending = functools.partial(send, k, 2, side, here, r3[k].at[d, m], out3.at[k, d], in3.at[k, d, m])
        if pending is not None:
            pending()

    swaps = [
        pltpu.make_async_remote_copy(
            src_ref=out[k].at[core], dst_ref=out[k].at[core], send_sem=swap_out.at[k], recv_sem=swap_in.at[k],
            device_id=partner, device_id_type=MESH,
        )
        for k in WEIGHTS
    ]
    for swap in swaps:
        swap.start()
    for k in WEIGHTS:
        pltpu.make_async_copy(part[k], part[k], part_out.at[k]).wait()
        for d in range(2):
            arrived(r1[k].at[d], out1.at[k, d])
            arrived(r2[k].at[d], out2.at[k, d])
            arrived(r3[k].at[d], out3.at[k, d])
    for k, swap in zip(WEIGHTS, swaps, strict=True):
        swap.wait_send()
        arrived(out[k].at[1 - core], swap_in.at[k])


def gather_kernel(*refs):
    new, own, other = refs[0:3], refs[3:6], refs[6:9]
    theirs = refs[9:11]
    in1, out1, in2, out2, in3, out3, pass_in, pass_out, swap_in, swap_out = refs[11:]
    chip, core = place()
    partner = device(chip, 1 - core)
    at = [[chip[axis] for axis in ORDER[k]] for k in WEIGHTS]
    lanes = [(k, d, side) for d, side in enumerate(SIDES) for k in WEIGHTS]
    greet(chip, core)

    def arrived(ref, sem):
        pltpu.make_async_copy(ref, ref, sem).wait()

    p, q, r = zip(*at, strict=True)
    landing = [theirs[0], theirs[1], own[2].at[p[2], q[2], core, r[2]]]
    for k in WEIGHTS:
        pltpu.make_async_remote_copy(
            src_ref=new[k].at[1 - core], dst_ref=landing[k], send_sem=swap_out.at[k], recv_sem=swap_in.at[k],
            device_id=partner, device_id_type=MESH,
        ).start()
    own[2][p[2], q[2], core, r[2]] = new[2][core]
    for k in range(2):
        arrived(theirs[k], swap_in.at[k])
        half = own[k].shape[-1]
        for h in range(2):
            columns = pl.ds(h * half, half)
            mine, yours = new[k][core, :, columns], theirs[k][:, columns]
            low, high = jnp.where(core == 0, mine, yours), jnp.where(core == 0, yours, mine)
            own[k][p[k], q[k], h, r[k]] = jnp.concatenate([low, high], axis=0).astype(jnp.bfloat16)
    arrived(own[2].at[p[2], q[2], 1 - core, r[2]], swap_in.at[2])

    def send(k, axis, side, ref, out_sem, in_sem):
        pltpu.make_async_remote_copy(
            src_ref=ref, dst_ref=ref, send_sem=out_sem, recv_sem=in_sem,
            device_id=neighbour(chip, core, ORDER[k][axis], side), device_id_type=MESH,
        ).start()

    def source(mine, side, m):
        return mine if m < 2 else lax.rem(mine - side + N, N)

    def send3(k, d, side, m):
        i3, h = source(r[k], side, m), half_of(side, m)
        send(k, 2, side, own[k].at[p[k], q[k], h, i3], out3.at[k, d], in3.at[k, d, m])

    def send2(k, d, side, m, i3):
        i2, h = source(q[k], side, m), half_of(side, m)
        send(k, 1, side, own[k].at[p[k], i2, h, i3], out2.at[k, d], in2.at[k, d, m, i3])

    def send1(k, d, side, m, i2):
        i1, h = source(p[k], side, m), half_of(side, m)
        send(k, 0, side, own[k].at[i1, i2, h], out1.at[k, d], in1.at[k, d, m, i2])

    def await3(k, d, m):
        arrived(r_block(k), in3.at[k, d, m])

    def await2(k, d, m, i3):
        arrived(r_block(k), in2.at[k, d, m, i3])

    def await1(k, d, m, i2):
        arrived(own[k].at[0, 0, 0], in1.at[k, d, m, i2])

    def r_block(k):
        return own[k].at[0, 0, 0, 0]

    def hand(k, i1, i2):
        pltpu.make_async_remote_copy(
            src_ref=own[k].at[i1, i2], dst_ref=other[k].at[i1, i2], send_sem=pass_out.at[k], recv_sem=pass_in.at[k],
            device_id=partner, device_id_type=MESH,
        ).start()

    def step(mine, offset):
        return lax.rem(mine + offset + N, N)

    for m in range(2):
        for k, d, side in lanes:
            send3(k, d, side, m)
    for m in range(2):
        for k, d, side in lanes:
            send2(k, d, side, m, r[k])
    for k, d, side in lanes:
        await3(k, d, 0)
        send3(k, d, side, 2)
    for behind in SIDES:
        e = SIDES.index(behind)
        for k in WEIGHTS:
            await3(k, e, 1)
        for m in range(2):
            for k, d, side in lanes:
                send2(k, d, side, m, step(r[k], -behind))
    for k, d, side in lanes:
        await3(k, d, 2)
    for m in range(2):
        for k, d, side in lanes:
            send2(k, d, side, m, step(r[k], 2))
    for m in range(2):
        for k, d, side in lanes:
            send1(k, d, side, m, q[k])
    for k in WEIGHTS:
        hand(k, p[k], q[k])
    for offset in (0, -1, 1, 2):
        for k, d, side in lanes:
            await2(k, d, 0, step(r[k], offset))
            send2(k, d, side, 2, step(r[k], offset))
    for behind in SIDES:
        e = SIDES.index(behind)
        for offset in (0, -1, 1, 2):
            for k in WEIGHTS:
                await2(k, e, 1, step(r[k], offset))
        for m in range(2):
            for k, d, side in lanes:
                send1(k, d, side, m, step(q[k], -behind))
        for k in WEIGHTS:
            hand(k, p[k], step(q[k], -behind))
    for offset in (0, -1, 1, 2):
        for k, d, side in lanes:
            await2(k, d, 2, step(r[k], offset))
    for m in range(2):
        for k, d, side in lanes:
            send1(k, d, side, m, step(q[k], 2))
    for k in WEIGHTS:
        hand(k, p[k], step(q[k], 2))
    for offset in (0, -1, 1, 2):
        for k, d, side in lanes:
            await1(k, d, 0, step(q[k], offset))
            send1(k, d, side, 2, step(q[k], offset))
    for offset in (0, -1, 1, 2):
        for k, d, side in lanes:
            await1(k, d, 1, step(q[k], offset))
            hand(k, step(p[k], -side), step(q[k], offset))
    for offset in (0, -1, 1, 2):
        for k in WEIGHTS:
            for d in range(2):
                await1(k, d, 2, step(q[k], offset))
            hand(k, step(p[k], 2), step(q[k], offset))

    for k in WEIGHTS:
        arrived(new[k].at[0], swap_out.at[k])
        for d in range(2):
            arrived(own[k].at[0:3, :, 0], out1.at[k, d])
            arrived(own[k].at[0, 0:3, 0], out2.at[k, d])
            arrived(own[k].at[0, 0, 0, 0:3], out3.at[k, d])
        arrived(own[k], pass_out.at[k])
        arrived(other[k], pass_in.at[k])


def write_kernel(*refs):
    own, other, out, sem = refs[0:3], refs[3:6], refs[6:9], refs[9]
    _, core = place()
    copies = []
    for i1 in range(N):
        for i2 in range(N):
            for h in range(2):
                for k in WEIGHTS:
                    copies.append(pltpu.make_async_copy(own[k].at[i1, i2, h], piece(out[k], k, core, i1, i2, h), sem.at[k, 0]))
                    copies.append(pltpu.make_async_copy(other[k].at[i1, i2, h], piece(out[k], k, 1 - core, i1, i2, h), sem.at[k, 1]))
    for copy in copies:
        copy.start()
    for k in WEIGHTS:
        pltpu.make_async_copy(own[k], own[k], sem.at[k, 0]).wait()
        pltpu.make_async_copy(other[k], other[k], sem.at[k, 1]).wait()


ANY = pl.BlockSpec(memory_space=pl.ANY)
VMEM = pl.BlockSpec(memory_space=pltpu.VMEM)
LIMIT = 67_000_000
SMALL = 4 * 2**20


def scatter(terms):
    bf16, dma = jnp.bfloat16, pltpu.SemaphoreType.DMA
    blocks = [(t.shape[-2], t.shape[-1] // 2) if k < 2 else t.shape[-2:] for k, t in enumerate(terms)]
    each = lambda *lead: [pltpu.VMEM((*lead, *b), bf16) for b in blocks]
    return pl.pallas_call(
        scatter_kernel,
        out_shape=[jax.ShapeDtypeStruct((2, 2, *b), bf16) for b in blocks],
        in_specs=[ANY] * 3,
        out_specs=[VMEM] * 3,
        scratch_shapes=[
            *each(N, N, 2, N), *each(2, 3, N, N), *each(2, 3, N), *each(2, 3), *each(2, 2, N), *each(N, 2, N),
            dma((3, N, N, 2)), dma((3,)),
            dma((3, 2, 3, N)), dma((3, 2)),
            dma((3, 2, 3, N)), dma((3, 2)),
            dma((3, 2, 3)), dma((3, 2)),
            dma((3, 2, 2)), dma((3,)), dma((3,)), dma((3,)),
        ],
        compiler_params=pltpu.CompilerParams(collective_id=0, has_side_effects=True, vmem_limit_bytes=LIMIT),
        name="scatter",
    )(*terms)


def gather(new):
    bf16, dma = jnp.bfloat16, pltpu.SemaphoreType.DMA
    blocks = [(2 * n.shape[1], n.shape[2] // 2) if k < 2 else n.shape[1:] for k, n in enumerate(new)]
    whole = [pltpu.VMEM((N, N, 2, N, *b), bf16) for b in blocks]
    return pl.pallas_call(
        gather_kernel,
        out_shape=whole * 2,
        in_specs=[VMEM] * 3,
        out_specs=[VMEM] * 6,
        scratch_shapes=[
            *(pltpu.VMEM(n.shape[1:], n.dtype) for n in new[:2]),
            dma((3, 2, 3, N)), dma((3, 2)),
            dma((3, 2, 3, N)), dma((3, 2)),
            dma((3, 2, 3)), dma((3, 2)),
            dma((3,)), dma((3,)), dma((3,)), dma((3,)),
        ],
        compiler_params=pltpu.CompilerParams(collective_id=1, has_side_effects=True, vmem_limit_bytes=SMALL),
        name="gather",
    )(*new)


def write(gathered, shapes):
    return pl.pallas_call(
        write_kernel,
        out_shape=[jax.ShapeDtypeStruct(s, jnp.bfloat16) for s in shapes],
        in_specs=[VMEM] * 6,
        out_specs=[ANY] * 3,
        scratch_shapes=[pltpu.SemaphoreType.DMA((3, 2))],
        compiler_params=pltpu.CompilerParams(vmem_limit_bytes=SMALL),
        name="write",
    )(*gathered)


def solution(mesh):
    def step(*arrays):
        terms, weights, m, v = (arrays[i : i + 3] for i in (0, 3, 6, 9))
        core = lax.rem(lax.axis_index("dp"), 2)
        me = lax.axis_index("dp")
        views = []
        for k, t in enumerate(terms):
            _, layers, rows, columns = t.shape
            block = rows // N**3
            views.append((layers, N, N, N, block, columns) if k < 2 else (layers, N, N, N, 2, block // 2, columns))
        sums = scatter([t.reshape(view) for t, view in zip(terms, views, strict=True)])
        gradients = []
        for k, total in enumerate(sums):
            if k < 2:
                layers, _, rows, half = total.shape
                total = total.transpose(0, 2, 1, 3).reshape(layers, 2, rows // 2, 2 * half)
            gradients.append(lax.dynamic_index_in_dim(total, core, 1, keepdims=False).astype(jnp.float32))
        own = [lax.dynamic_slice_in_dim(w, me * one.shape[1], one.shape[1], 1).astype(jnp.float32) for w, one in zip(weights, m, strict=True)]
        new = [adamw(*one) for one in zip(own, m, v, gradients, strict=True)]
        rows = [one[0].astype(jnp.bfloat16).astype(jnp.float32) if k < 2 else one[0].astype(jnp.bfloat16) for k, one in enumerate(new)]
        whole = write(gather(rows), views)
        whole = [w.reshape(t.shape[1:]) for w, t in zip(whole, terms, strict=True)]
        return (*whole, *(one[1] for one in new), *(one[2] for one in new))

    all_of, cut = P(None, None, None), P(None, "dp", None)
    return jax.shard_map(
        step,
        mesh=mesh,
        in_specs=(P(("rep", "dp"), None, None, None),) * 3 + (all_of,) * 3 + (cut,) * 6,
        out_specs=(P("rep", None, None),) * 3 + (P("rep", "dp", None),) * 6,
        check_vma=False,
    )
```

```python
import functools

import jax
import jax.numpy as jnp
from jax import lax
from jax.experimental import pallas as pl
from jax.experimental.pallas import tpu as pltpu
from jax.sharding import PartitionSpec as P

N = 4
MESH = pl.DeviceIdType.MESH
ORDER = ((0, 1, 2), (1, 2, 0), (2, 0, 1))
SIDES = (1, -1)
WEIGHTS = range(3)


def adamw(w, m, v, g):
    m = 0.9 * m + 0.1 * g
    v = 0.95 * v + 0.05 * g * g
    step = m * lax.rsqrt(v + 1e-8) + 0.1 * w
    return w - 0.02 * step, m, v


def place():
    me = lax.axis_index("dp")
    core = lax.rem(me, 2)
    chip = me // 2
    return (chip // (N * N), lax.rem(chip // N, N), lax.rem(chip, N)), core


def device(chip, core):
    return {"dp": ((chip[0] * N + chip[1]) * N + chip[2]) * 2 + core}


def neighbour(chip, core, axis, side):
    moved = list(chip)
    moved[axis] = lax.rem(chip[axis] + side + N, N)
    return device(moved, core)


def greet(chip, core):
    barrier = pltpu.get_barrier_semaphore()
    others = [device(chip, 1 - core)] + [neighbour(chip, core, axis, side) for axis in range(3) for side in SIDES]
    for other in others:
        pl.semaphore_signal(barrier, inc=1, device_id=other, device_id_type=MESH)
    pl.semaphore_wait(barrier, len(others))


def piece(ref, k, layer, i1, i2, h):
    if k == 2:
        return ref.at[layer, i2, :, i1, h]
    half = ref.shape[-1] // 2
    columns = pl.ds(pl.multiple_of(h * half, half), half)
    if k == 0:
        return ref.at[layer, i1, i2, :, :, columns]
    return ref.at[layer, :, i1, i2, :, columns]


def far(m):
    return (4 - m) // 2


def half_of(side, m):
    h = lax.rem(m, 2) * (1 - m // 2) if not isinstance(m, int) else (m % 2) * (1 - m // 2)
    return h if side == 1 else 1 - h


def target(mine, side, m):
    return lax.rem(mine + side * far(m) + N, N)


def turn(mine, s):
    return lax.rem(mine + 2 - s + (s // 2) * (2 * s - 1) + N, N)


def put_sum(out, sources):
    def one(out, sources):
        total = sources[0][...].astype(jnp.float32)
        for source in sources[1:]:
            total = total + source[...].astype(jnp.float32)
        out[...] = total.astype(out.dtype)

    if len(out.shape) == 2:
        one(out, sources)
    else:

        @pl.loop(0, out.shape[0])
        def _(i):
            one(out.at[i], [source.at[i] for source in sources])


def rows_of_both(core, mine, theirs):
    low, high = jnp.where(core == 0, mine, theirs), jnp.where(core == 0, theirs, mine)
    return jnp.concatenate([low, high], axis=0)


def step_kernel(*refs):
    g, w, moments = refs[0:3], refs[3:6], (refs[6:9], refs[9:12])
    own, other, fresh = refs[12:15], refs[15:18], (refs[18:21], refs[21:24])
    ahead, kept, grad, weight = (refs[24 + 3 * i : 27 + 3 * i] for i in range(4))
    mine, theirs = ((refs[36 + 6 * i : 39 + 6 * i], refs[39 + 6 * i : 42 + 6 * i]) for i in range(2))
    part_in, part_out, rs1_in, rs1_out, rs2_in, rs2_out, rs3_in, rs3_out, ahead_in, kept_in = refs[48:58]
    weight_in, mine_in, theirs_in, theirs_out, grad_in, grad_out = refs[58:64]
    in1, out1, in2, out2, in3, out3, pass_in, pass_out, ready = refs[64:73]
    chip, core = place()
    partner = device(chip, 1 - core)
    at = [[chip[axis] for axis in ORDER[k]] for k in WEIGHTS]
    p, q, r = zip(*at, strict=True)
    lanes = [(k, d, side) for d, side in enumerate(SIDES) for k in WEIGHTS]

    def flat(i1, i2, h):
        return (i1 * N + i2) * 2 + h

    def arrived(ref, sem):
        pltpu.make_async_copy(ref, ref, sem).wait()

    def push(src, dst, out_sem, in_sem, where):
        pltpu.make_async_remote_copy(
            src_ref=src, dst_ref=dst, send_sem=out_sem, recv_sem=in_sem, device_id=where, device_id_type=MESH
        ).start()

    def send(k, axis, side, src, dst, out_sem, in_sem):
        push(src, dst, out_sem, in_sem, neighbour(chip, core, ORDER[k][axis], side))

    def r1(k, d, m, i2):
        return other[k].at[(d * 3 + m) * N + i2]

    def r2(k, d, m, i3):
        return other[k].at[24 + d * 3 + m, i3]

    def r3(k, d, m):
        return other[k].at[30 + d, m]

    def spot(k, side, t):
        m, s = t // N, lax.rem(t, N)
        return target(p[k], side, m), turn(q[k], s), half_of(side, m)

    def give(t):
        for k, d, side in lanes:
            i1, i2, h = spot(k, side, t)
            push(piece(g[k], k, 1 - core, i1, i2, h), own[k].at[flat(i1, i2, h)], part_out.at[k], part_in.at[k, flat(i1, i2, h)], partner)

    def fetch(t):
        for k, d, side in lanes:
            i1, i2, h = spot(k, side, t)
            slot = lax.rem(t, 2)
            yield pltpu.make_async_copy(piece(g[k], k, core, i1, i2, h), ahead[k].at[slot, d], ahead_in.at[k, slot, d])

    def part_arrived(k, i1, i2, h):
        arrived(own[k].at[flat(i1, i2, h)], part_in.at[k, flat(i1, i2, h)])

    small = [pltpu.make_async_copy(w[k].at[core, chip[0], chip[1], chip[2]], weight[k], weight_in.at[k]) for k in WEIGHTS]
    small += [pltpu.make_async_copy(moments[i][k], mine[i][k], mine_in.at[i, k]) for i in range(2) for k in WEIGHTS]
    for copy in fetch(0):
        copy.start()
    greet(chip, core)

    @pl.loop(0, N)
    def _(t):
        give(t)

    for copy in small:
        copy.start()
    for i in range(2):
        for k in WEIGHTS:
            push(moments[i][k].at[1 - core], theirs[i][k], theirs_out.at[i, k], theirs_in.at[i, k], partner)

    def first(last):
        def body(t):
            give(t + N)
            if last:

                @pl.when(t + 1 < 3 * N)
                def _():
                    for copy in fetch(t + 1):
                        copy.start()
            else:
                for copy in fetch(t + 1):
                    copy.start()
            pending = None
            for (k, d, side), copy in zip(lanes, fetch(t), strict=True):
                i1, i2, h = spot(k, side, t)
                copy.wait()
                part_arrived(k, i1, i2, h)
                here = own[k].at[flat(i1, i2, h)]
                sources = [here, ahead[k].at[lax.rem(t, 2), d]]
                if last:
                    arrived(r1(k, d, 0, i2), rs1_in.at[k, d, 0, i2])
                    sources.append(r1(k, d, 0, i2))
                put_sum(here, sources)
                if pending is not None:
                    pending()
                m = 2 if last else t // N
                pending = functools.partial(send, k, 0, side, here, r1(k, d, m, i2), rs1_out.at[k, d], rs1_in.at[k, d, m, i2])
            pending()

        return body

    pl.loop(0, 2 * N)(first(False))
    for k in WEIGHTS:
        for i2 in range(N):
            for h in range(2):
                pltpu.make_async_copy(piece(g[k], k, core, p[k], i2, h), kept[k].at[i2, h], kept_in.at[k]).start()
    pl.loop(2 * N, 3 * N)(first(True))

    for k in WEIGHTS:
        arrived(kept[k], kept_in.at[k])

    def settled(k, side, m):
        i2, h = target(q[k], side, m), half_of(side, m)
        part_arrived(k, p[k], i2, h)
        for d, m1 in ((0, 2 - h), (1, 1 + h)):
            arrived(r1(k, d, m1, i2), rs1_in.at[k, d, m1, i2])

    def terms(k, i2, h, i3):
        here = own[k].at[flat(p[k], i2, h), i3]
        return here, [here, kept[k].at[i2, h, i3], r1(k, 0, 2 - h, i2).at[i3], r1(k, 1, 1 + h, i2).at[i3]]

    for m in range(3):
        for k, d, side in lanes:
            settled(k, side, m)

        @pl.loop(0, N)
        def _(s):
            pending = None
            for k, d, side in lanes:
                i2, h, i3 = target(q[k], side, m), half_of(side, m), turn(r[k], s)
                here, sources = terms(k, i2, h, i3)
                if m == 2:
                    arrived(r2(k, d, 0, i3), rs2_in.at[k, d, 0, i3])
                    sources.append(r2(k, d, 0, i3))
                put_sum(here, sources)
                if pending is not None:
                    pending()
                pending = functools.partial(send, k, 1, side, here, r2(k, d, m, i3), rs2_out.at[k, d], rs2_in.at[k, d, m, i3])
            pending()

    for copy in small:
        copy.wait()
    for i in range(2):
        for k in WEIGHTS:
            arrived(theirs[i][k], theirs_in.at[i, k])
    for k, d, side in lanes:
        settled(k, side, 3)
    for m in range(4):
        pending = None
        for k, d, side in lanes:
            h, i3 = half_of(side, m), target(r[k], side, m)
            here, sources = terms(k, q[k], h, i3)
            for e, m2 in ((0, 2 - h), (1, 1 + h)):
                arrived(r2(k, e, m2, i3), rs2_in.at[k, e, m2, i3])
                sources.append(r2(k, e, m2, i3))
            if m == 2:
                arrived(r3(k, d, 0), rs3_in.at[k, d, 0])
                sources.append(r3(k, d, 0))
            if m == 3:
                for e, m3 in ((0, 2 - h), (1, 1 + h)):
                    arrived(r3(k, e, m3), rs3_in.at[k, e, m3])
                    sources.append(r3(k, e, m3))
                here = grad[k].at[core, h]
            put_sum(here, sources)
            if pending is not None:
                pending()
            pending = None
            if m < 3:
                pending = functools.partial(send, k, 2, side, here, r3(k, d, m), rs3_out.at[k, d], rs3_in.at[k, d, m])
        if pending is not None:
            pending()

    for k in WEIGHTS:
        for d in range(2):
            arrived(own[k].at[0:12], rs1_out.at[k, d])
            arrived(own[k].at[0:3], rs2_out.at[k, d])
            arrived(own[k].at[0, 0:3], rs3_out.at[k, d])
    for where in [partner] + [neighbour(chip, core, axis, side) for axis in range(3) for side in SIDES]:
        pl.semaphore_signal(ready, inc=1, device_id=where, device_id_type=MESH)

    for k in range(2):
        half = own[k].shape[-1]
        width = min(half, 1024)
        for h in range(2):
            block = own[k].at[flat(p[k], q[k], h), r[k]]

            @pl.loop(0, half // width)
            def _(c):
                within = pl.ds(pl.multiple_of(c * width, width), width)
                columns = pl.ds(pl.multiple_of(h * half + c * width, width), width)
                m, v = (rows_of_both(core, mine[i][k][core, :, columns], theirs[i][k][:, columns]) for i in range(2))
                new, _, _ = adamw(weight[k][:, columns].astype(jnp.float32), m, v, grad[k][core, h, :, within].astype(jnp.float32))
                block[:, within] = new.astype(block.dtype)

    depth = min(own[2].shape[-2], 16)
    for h in range(2):
        block = own[2].at[flat(p[2], q[2], h), r[2]]

        @pl.loop(0, own[2].shape[-2] // depth)
        def _(c):
            rows = pl.ds(pl.multiple_of(c * depth, depth), depth)
            m, v = (jnp.where(core == h, mine[i][2][core, rows], theirs[i][2][rows]) for i in range(2))
            new, _, _ = adamw(weight[2][h, rows].astype(jnp.float32), m, v, grad[2][core, h, rows].astype(jnp.float32))
            block[rows] = new.astype(block.dtype)

    for k in WEIGHTS:
        push(grad[k].at[core], grad[k].at[core], grad_out.at[k], grad_in.at[k], partner)
    pl.semaphore_wait(ready, 7)

    def source(mine, side, m):
        return mine if m < 2 else lax.rem(mine - side + N, N)

    def send3(k, d, side, m):
        i3, h = source(r[k], side, m), half_of(side, m)
        ref = own[k].at[flat(p[k], q[k], h), i3]
        send(k, 2, side, ref, ref, out3.at[k, d], in3.at[k, d, m])

    def send2(k, d, side, m, i3):
        i2, h = source(q[k], side, m), half_of(side, m)
        ref = own[k].at[flat(p[k], i2, h), i3]
        send(k, 1, side, ref, ref, out2.at[k, d], in2.at[k, d, m, i3])

    def send1(k, d, side, m, i2):
        i1, h = source(p[k], side, m), half_of(side, m)
        ref = own[k].at[flat(i1, i2, h)]
        send(k, 0, side, ref, ref, out1.at[k, d], in1.at[k, d, m, i2])

    def await3(k, d, m):
        arrived(own[k].at[0, 0], in3.at[k, d, m])

    def await2(k, d, m, i3):
        arrived(own[k].at[0, 0], in2.at[k, d, m, i3])

    def await1(k, d, m, i2):
        arrived(own[k].at[0], in1.at[k, d, m, i2])

    def hand(k, i1, i2):
        both = pl.ds(flat(i1, i2, 0), 2)
        push(own[k].at[both], other[k].at[both], pass_out.at[k], pass_in.at[k], partner)

    def step(mine, offset):
        return lax.rem(mine + offset + N, N)

    for m in range(2):
        for k, d, side in lanes:
            send3(k, d, side, m)
    for m in range(2):
        for k, d, side in lanes:
            send2(k, d, side, m, r[k])
    for k, d, side in lanes:
        await3(k, d, 0)
        send3(k, d, side, 2)
    for e, behind in enumerate(SIDES):
        for k in WEIGHTS:
            await3(k, e, 1)
        for m in range(2):
            for k, d, side in lanes:
                send2(k, d, side, m, step(r[k], -behind))
    for k, d, side in lanes:
        await3(k, d, 2)
    for m in range(2):
        for k, d, side in lanes:
            send2(k, d, side, m, step(r[k], 2))
    for m in range(2):
        for k, d, side in lanes:
            send1(k, d, side, m, q[k])
    for k in WEIGHTS:
        hand(k, p[k], q[k])

    for k in WEIGHTS:
        arrived(grad[k].at[1 - core], grad_in.at[k])
    for layer in range(2):
        for k in range(2):
            half = own[k].shape[-1]
            width = min(half, 1024)
            for h in range(2):

                @pl.loop(0, half // width)
                def _(c):
                    within = pl.ds(pl.multiple_of(c * width, width), width)
                    columns = pl.ds(pl.multiple_of(h * half + c * width, width), width)
                    total = grad[k][layer, h, :, within].astype(jnp.float32)
                    rows = total.shape[0] // 2
                    total = jnp.where(core == 0, total[:rows], total[rows:])
                    _, m, v = adamw(total, mine[0][k][layer, :, columns], mine[1][k][layer, :, columns], total)
                    fresh[0][k][layer, :, columns] = m
                    fresh[1][k][layer, :, columns] = v

        @pl.loop(0, own[2].shape[-2] // depth)
        def _(c):
            rows = pl.ds(pl.multiple_of(c * depth, depth), depth)
            total = grad[2][layer, core, rows].astype(jnp.float32)
            _, m, v = adamw(total, mine[0][2][layer, rows], mine[1][2][layer, rows], total)
            fresh[0][2][layer, rows] = m
            fresh[1][2][layer, rows] = v

    for offset in (0, -1, 1, 2):
        for k, d, side in lanes:
            await2(k, d, 0, step(r[k], offset))
            send2(k, d, side, 2, step(r[k], offset))
    for e, behind in enumerate(SIDES):
        for offset in (0, -1, 1, 2):
            for k in WEIGHTS:
                await2(k, e, 1, step(r[k], offset))
        for m in range(2):
            for k, d, side in lanes:
                send1(k, d, side, m, step(q[k], -behind))
        for k in WEIGHTS:
            hand(k, p[k], step(q[k], -behind))
    for offset in (0, -1, 1, 2):
        for k, d, side in lanes:
            await2(k, d, 2, step(r[k], offset))
    for m in range(2):
        for k, d, side in lanes:
            send1(k, d, side, m, step(q[k], 2))
    for k in WEIGHTS:
        hand(k, p[k], step(q[k], 2))
    for offset in (0, -1, 1, 2):
        for k, d, side in lanes:
            await1(k, d, 0, step(q[k], offset))
            send1(k, d, side, 2, step(q[k], offset))
    for offset in (0, -1, 1, 2):
        for k, d, side in lanes:
            await1(k, d, 1, step(q[k], offset))
            hand(k, step(p[k], -side), step(q[k], offset))
    for offset in (0, -1, 1, 2):
        for k in WEIGHTS:
            for d in range(2):
                await1(k, d, 2, step(q[k], offset))
            hand(k, step(p[k], 2), step(q[k], offset))

    for k in WEIGHTS:
        arrived(own[k], part_out.at[k])
        arrived(grad[k].at[0], grad_out.at[k])
        for i in range(2):
            arrived(theirs[i][k], theirs_out.at[i, k])
        for d in range(2):
            arrived(own[k].at[0:12], out1.at[k, d])
            arrived(own[k].at[0:3], out2.at[k, d])
            arrived(own[k].at[0, 0:3], out3.at[k, d])
        arrived(own[k], pass_out.at[k])
        arrived(other[k], pass_in.at[k])


def write_kernel(*refs):
    own, other, moments, out, written, sem, moment_sem = refs[0:3], refs[3:6], refs[6:12], refs[12:15], refs[15:21], refs[21], refs[22]
    _, core = place()
    copies = []
    for i1 in range(N):
        for i2 in range(N):
            for h in range(2):
                for k in WEIGHTS:
                    j = (i1 * N + i2) * 2 + h
                    copies.append(pltpu.make_async_copy(own[k].at[j], piece(out[k], k, core, i1, i2, h), sem.at[k, 0]))
                    copies.append(pltpu.make_async_copy(other[k].at[j], piece(out[k], k, 1 - core, i1, i2, h), sem.at[k, 1]))
    small = [pltpu.make_async_copy(a, b, moment_sem.at[i]) for i, (a, b) in enumerate(zip(moments, written, strict=True))]
    for copy in copies + small:
        copy.start()
    for k in WEIGHTS:
        pltpu.make_async_copy(own[k], own[k], sem.at[k, 0]).wait()
        pltpu.make_async_copy(other[k], other[k], sem.at[k, 1]).wait()
    for copy in small:
        copy.wait()


ANY = pl.BlockSpec(memory_space=pl.ANY)
VMEM = pl.BlockSpec(memory_space=pltpu.VMEM)
LIMIT = 14 * 2**20
SMALL = 2**20


def solution(mesh):
    bf16, f32, dma = jnp.bfloat16, jnp.float32, pltpu.SemaphoreType.DMA

    def step(*arrays):
        terms, weights, m, v = (arrays[i : i + 3] for i in (0, 3, 6, 9))
        views, blocks = [], []
        for k, w in enumerate(weights):
            layers, rows, columns = w.shape
            block = rows // N**3
            views.append((layers, N, N, N, block, columns) if k < 2 else (layers, N, N, N, 2, block // 2, columns))
            blocks.append((block, columns // 2) if k < 2 else (block // 2, columns))
        each = lambda *lead: [pltpu.VMEM((*lead, *b), bf16) for b in blocks]
        moment = [pltpu.VMEM(one.shape, f32) for one in (*m, *v)]
        layer = [pltpu.VMEM(one.shape[1:], f32) for one in (*m, *v)]
        results = pl.pallas_call(
            step_kernel,
            out_shape=[*each(2 * N * N, N), *each(2 * N * N, N), *moment],
            in_specs=[ANY] * 12,
            out_specs=[VMEM] * 12,
            scratch_shapes=[
                *each(2, 2, N), *each(N, 2, N), *each(2, 2), *(pltpu.VMEM(view[4:], bf16) for view in views),
                *moment, *layer,
                dma((3, 2 * N * N)), dma((3,)),
                dma((3, 2, 3, N)), dma((3, 2)),
                dma((3, 2, 3, N)), dma((3, 2)),
                dma((3, 2, 3)), dma((3, 2)),
                dma((3, 2, 2)), dma((3,)),
                dma((3,)), dma((2, 3)), dma((2, 3)), dma((2, 3)), dma((3,)), dma((3,)),
                dma((3, 2, 3, N)), dma((3, 2)),
                dma((3, 2, 3, N)), dma((3, 2)),
                dma((3, 2, 3)), dma((3, 2)),
                dma((3,)), dma((3,)), pltpu.SemaphoreType.REGULAR,
            ],
            compiler_params=pltpu.CompilerParams(collective_id=0, has_side_effects=True, vmem_limit_bytes=LIMIT),
            name="step",
        )(*(t.reshape(view) for t, view in zip(terms, views, strict=True)), *(w.reshape(view) for w, view in zip(weights, views, strict=True)), *m, *v)
        out = pl.pallas_call(
            write_kernel,
            out_shape=[*(jax.ShapeDtypeStruct(view, bf16) for view in views), *(jax.ShapeDtypeStruct(one.shape, f32) for one in (*m, *v))],
            in_specs=[VMEM] * 12,
            out_specs=[ANY] * 9,
            scratch_shapes=[dma((3, 2)), dma((6,))],
            compiler_params=pltpu.CompilerParams(vmem_limit_bytes=SMALL),
            name="write",
        )(*results)
        return (*(w.reshape(old.shape) for w, old in zip(out[:3], weights, strict=True)), *out[3:])

    all_of, cut = P(None, None, None), P(None, "dp", None)
    return jax.shard_map(
        step,
        mesh=mesh,
        in_specs=(P(("rep", "dp"), None, None, None),) * 3 + (all_of,) * 3 + (cut,) * 6,
        out_specs=(P("rep", None, None),) * 3 + (P("rep", "dp", None),) * 6,
        check_vma=False,
    )
```

```python
import functools

import jax
import jax.numpy as jnp
from jax import lax
from jax.experimental import pallas as pl
from jax.experimental.pallas import tpu as pltpu
from jax.sharding import PartitionSpec as P

N = 4
MESH = pl.DeviceIdType.MESH
ORDER = ((0, 1, 2), (1, 2, 0), (2, 0, 1))
SIDES = (1, -1)
WEIGHTS = range(3)


def adamw(w, m, v, g):
    m = 0.9 * m + 0.1 * g
    v = 0.95 * v + 0.05 * g * g
    step = m * lax.rsqrt(v + 1e-8) + 0.1 * w
    return w - 0.02 * step, m, v


def place():
    me = lax.axis_index("dp")
    core = lax.rem(me, 2)
    chip = me // 2
    return (chip // (N * N), lax.rem(chip // N, N), lax.rem(chip, N)), core


def device(chip, core):
    return {"dp": ((chip[0] * N + chip[1]) * N + chip[2]) * 2 + core}


def neighbour(chip, core, axis, side):
    moved = list(chip)
    moved[axis] = lax.rem(chip[axis] + side + N, N)
    return device(moved, core)


def greet(chip, core):
    barrier = pltpu.get_barrier_semaphore()
    others = [device(chip, 1 - core)] + [neighbour(chip, core, axis, side) for axis in range(3) for side in SIDES]
    for other in others:
        pl.semaphore_signal(barrier, inc=1, device_id=other, device_id_type=MESH)
    pl.semaphore_wait(barrier, len(others))


def piece(ref, k, layer, i1, i2, h):
    if k == 2:
        return ref.at[layer, i2, :, i1, h]
    half = ref.shape[-1] // 2
    columns = pl.ds(pl.multiple_of(h * half, half), half)
    if k == 0:
        return ref.at[layer, i1, i2, :, :, columns]
    return ref.at[layer, :, i1, i2, :, columns]


def far(m):
    return (4 - m) // 2


def half_of(side, m):
    h = lax.rem(m, 2) * (1 - m // 2) if not isinstance(m, int) else (m % 2) * (1 - m // 2)
    return h if side == 1 else 1 - h


def target(mine, side, m):
    return lax.rem(mine + side * far(m) + N, N)


def turn(mine, s):
    return lax.rem(mine + 2 - s + (s // 2) * (2 * s - 1) + N, N)


def put_sum(out, sources):
    def one(out, sources):
        total = sources[0][...].astype(jnp.float32)
        for source in sources[1:]:
            total = total + source[...].astype(jnp.float32)
        out[...] = total.astype(out.dtype)

    if len(out.shape) == 2:
        one(out, sources)
    else:

        @pl.loop(0, out.shape[0])
        def _(i):
            one(out.at[i], [source.at[i] for source in sources])


def rows_of_both(core, mine, theirs):
    low, high = jnp.where(core == 0, mine, theirs), jnp.where(core == 0, theirs, mine)
    return jnp.concatenate([low, high], axis=0)


def step_kernel(*refs):
    g, w, moments = refs[0:3], refs[3:6], (refs[6:9], refs[9:12])
    own, other, fresh = refs[12:15], refs[15:18], (refs[18:21], refs[21:24])
    ahead, grad, weight = (refs[24 + 3 * i : 27 + 3 * i] for i in range(3))
    theirs = (refs[33:36], refs[36:39])
    part_in, part_out, rs1_in, rs1_out, rs2_in, rs2_out, rs3_in, rs3_out, ahead_in = refs[39:48]
    weight_in, fresh_in, theirs_in, theirs_out, grad_in, grad_out = refs[48:54]
    in1, out1, in2, out2, in3, out3, pass_in, pass_out, ready = refs[54:63]
    chip, core = place()
    partner = device(chip, 1 - core)
    at = [[chip[axis] for axis in ORDER[k]] for k in WEIGHTS]
    p, q, r = zip(*at, strict=True)
    lanes = [(k, d, side) for d, side in enumerate(SIDES) for k in WEIGHTS]

    def flat(i1, i2, h):
        return (i1 * N + i2) * 2 + h

    def arrived(ref, sem):
        pltpu.make_async_copy(ref, ref, sem).wait()

    def push(src, dst, out_sem, in_sem, where):
        pltpu.make_async_remote_copy(
            src_ref=src, dst_ref=dst, send_sem=out_sem, recv_sem=in_sem, device_id=where, device_id_type=MESH
        ).start()

    def send(k, axis, side, src, dst, out_sem, in_sem):
        push(src, dst, out_sem, in_sem, neighbour(chip, core, ORDER[k][axis], side))

    def r1(k, d, m, i2):
        return other[k].at[(d * 3 + m) * N + i2]

    def r2(k, d, m, i3):
        return other[k].at[24 + d * 3 + m, i3]

    def r3(k, d, m):
        return other[k].at[30 + d, m]

    def spot(k, side, t):
        m, s = t // N, lax.rem(t, N)
        return target(p[k], side, m), turn(q[k], s), half_of(side, m)

    def give(t):
        for k, d, side in lanes:
            i1, i2, h = spot(k, side, t)
            push(piece(g[k], k, 1 - core, i1, i2, h), own[k].at[flat(i1, i2, h)], part_out.at[k], part_in.at[k, flat(i1, i2, h)], partner)

    def fetch(t):
        for k, d, side in lanes:
            i1, i2, h = spot(k, side, t)
            slot = lax.rem(t, 2)
            yield pltpu.make_async_copy(piece(g[k], k, core, i1, i2, h), ahead[k].at[slot, d], ahead_in.at[k, slot, d])

    def part_arrived(k, i1, i2, h):
        arrived(own[k].at[flat(i1, i2, h)], part_in.at[k, flat(i1, i2, h)])

    small = [pltpu.make_async_copy(w[k].at[core, chip[0], chip[1], chip[2]], weight[k], weight_in.at[k]) for k in WEIGHTS]
    small += [pltpu.make_async_copy(moments[i][k], fresh[i][k], fresh_in.at[i, k]) for i in range(2) for k in WEIGHTS]
    for copy in fetch(0):
        copy.start()
    greet(chip, core)

    @pl.loop(0, N)
    def _(t):
        give(t)

    for copy in small:
        copy.start()
    for i in range(2):
        for k in WEIGHTS:
            push(moments[i][k].at[1 - core], theirs[i][k], theirs_out.at[i, k], theirs_in.at[i, k], partner)

    def first(last):
        def body(t):
            give(t + N)
            if last:

                @pl.when(t + 1 < 3 * N)
                def _():
                    for copy in fetch(t + 1):
                        copy.start()
            else:
                for copy in fetch(t + 1):
                    copy.start()
            pending = None
            for (k, d, side), copy in zip(lanes, fetch(t), strict=True):
                i1, i2, h = spot(k, side, t)
                copy.wait()
                part_arrived(k, i1, i2, h)
                here = own[k].at[flat(i1, i2, h)]
                sources = [here, ahead[k].at[lax.rem(t, 2), d]]
                if last:
                    arrived(r1(k, d, 0, i2), rs1_in.at[k, d, 0, i2])
                    sources.append(r1(k, d, 0, i2))
                put_sum(here, sources)
                if pending is not None:
                    pending()
                m = 2 if last else t // N
                pending = functools.partial(send, k, 0, side, here, r1(k, d, m, i2), rs1_out.at[k, d], rs1_in.at[k, d, m, i2])
            pending()

        return body

    pl.loop(0, 2 * N)(first(False))
    pl.loop(2 * N, 3 * N)(first(True))

    def fetch_kept(m):
        for k, d, side in lanes:
            i2, h = target(q[k], side, m), half_of(side, m)
            yield pltpu.make_async_copy(piece(g[k], k, core, p[k], i2, h), ahead[k].at[m % 2, d], ahead_in.at[k, m % 2, d])

    for copy in fetch_kept(0):
        copy.start()

    def settled(k, side, m):
        i2, h = target(q[k], side, m), half_of(side, m)
        part_arrived(k, p[k], i2, h)
        for d, m1 in ((0, 2 - h), (1, 1 + h)):
            arrived(r1(k, d, m1, i2), rs1_in.at[k, d, m1, i2])

    def terms(k, i2, h, i3, kept):
        here = own[k].at[flat(p[k], i2, h), i3]
        return here, [here, kept.at[i3], r1(k, 0, 2 - h, i2).at[i3], r1(k, 1, 1 + h, i2).at[i3]]

    for m in range(3):
        for (k, d, side), copy in zip(lanes, fetch_kept(m), strict=True):
            settled(k, side, m)
            copy.wait()
        for copy in fetch_kept(m + 1):
            copy.start()

        @pl.loop(0, N)
        def _(s):
            pending = None
            for k, d, side in lanes:
                i2, h, i3 = target(q[k], side, m), half_of(side, m), turn(r[k], s)
                here, sources = terms(k, i2, h, i3, ahead[k].at[m % 2, d])
                if m == 2:
                    arrived(r2(k, d, 0, i3), rs2_in.at[k, d, 0, i3])
                    sources.append(r2(k, d, 0, i3))
                put_sum(here, sources)
                if pending is not None:
                    pending()
                pending = functools.partial(send, k, 1, side, here, r2(k, d, m, i3), rs2_out.at[k, d], rs2_in.at[k, d, m, i3])
            pending()

    for copy in small:
        copy.wait()
    for i in range(2):
        for k in WEIGHTS:
            arrived(theirs[i][k], theirs_in.at[i, k])
    for (k, d, side), copy in zip(lanes, fetch_kept(3), strict=True):
        settled(k, side, 3)
        copy.wait()
    for m in range(4):
        pending = None
        for k, d, side in lanes:
            h, i3 = half_of(side, m), target(r[k], side, m)
            here, sources = terms(k, q[k], h, i3, ahead[k].at[1, h])
            for e, m2 in ((0, 2 - h), (1, 1 + h)):
                arrived(r2(k, e, m2, i3), rs2_in.at[k, e, m2, i3])
                sources.append(r2(k, e, m2, i3))
            if m == 2:
                arrived(r3(k, d, 0), rs3_in.at[k, d, 0])
                sources.append(r3(k, d, 0))
            if m == 3:
                for e, m3 in ((0, 2 - h), (1, 1 + h)):
                    arrived(r3(k, e, m3), rs3_in.at[k, e, m3])
                    sources.append(r3(k, e, m3))
                here = grad[k].at[core, h]
            put_sum(here, sources)
            if pending is not None:
                pending()
            pending = None
            if m < 3:
                pending = functools.partial(send, k, 2, side, here, r3(k, d, m), rs3_out.at[k, d], rs3_in.at[k, d, m])
        if pending is not None:
            pending()

    for k in WEIGHTS:
        for d in range(2):
            arrived(own[k].at[0:12], rs1_out.at[k, d])
            arrived(own[k].at[0:3], rs2_out.at[k, d])
            arrived(own[k].at[0, 0:3], rs3_out.at[k, d])
    for where in [partner] + [neighbour(chip, core, axis, side) for axis in range(3) for side in SIDES]:
        pl.semaphore_signal(ready, inc=1, device_id=where, device_id_type=MESH)

    for k in range(2):
        half = own[k].shape[-1]
        width = min(half, 1024)
        for h in range(2):
            block = own[k].at[flat(p[k], q[k], h), r[k]]

            @pl.loop(0, half // width)
            def _(c):
                within = pl.ds(pl.multiple_of(c * width, width), width)
                columns = pl.ds(pl.multiple_of(h * half + c * width, width), width)
                m, v = (rows_of_both(core, fresh[i][k][core, :, columns], theirs[i][k][:, columns]) for i in range(2))
                new, _, _ = adamw(weight[k][:, columns].astype(jnp.float32), m, v, grad[k][core, h, :, within].astype(jnp.float32))
                block[:, within] = new.astype(block.dtype)

    depth = min(own[2].shape[-2], 16)
    for h in range(2):
        block = own[2].at[flat(p[2], q[2], h), r[2]]

        @pl.loop(0, own[2].shape[-2] // depth)
        def _(c):
            rows = pl.ds(pl.multiple_of(c * depth, depth), depth)
            m, v = (jnp.where(core == h, fresh[i][2][core, rows], theirs[i][2][rows]) for i in range(2))
            new, _, _ = adamw(weight[2][h, rows].astype(jnp.float32), m, v, grad[2][core, h, rows].astype(jnp.float32))
            block[rows] = new.astype(block.dtype)

    for k in WEIGHTS:
        push(grad[k].at[core], grad[k].at[core], grad_out.at[k], grad_in.at[k], partner)
    pl.semaphore_wait(ready, 7)

    def source(mine, side, m):
        return mine if m < 2 else lax.rem(mine - side + N, N)

    def send3(k, d, side, m):
        i3, h = source(r[k], side, m), half_of(side, m)
        ref = own[k].at[flat(p[k], q[k], h), i3]
        send(k, 2, side, ref, ref, out3.at[k, d], in3.at[k, d, m])

    def send2(k, d, side, m, i3):
        i2, h = source(q[k], side, m), half_of(side, m)
        ref = own[k].at[flat(p[k], i2, h), i3]
        send(k, 1, side, ref, ref, out2.at[k, d], in2.at[k, d, m, i3])

    def send1(k, d, side, m, i2):
        i1, h = source(p[k], side, m), half_of(side, m)
        ref = own[k].at[flat(i1, i2, h)]
        send(k, 0, side, ref, ref, out1.at[k, d], in1.at[k, d, m, i2])

    def await3(k, d, m):
        arrived(own[k].at[0, 0], in3.at[k, d, m])

    def await2(k, d, m, i3):
        arrived(own[k].at[0, 0], in2.at[k, d, m, i3])

    def await1(k, d, m, i2):
        arrived(own[k].at[0], in1.at[k, d, m, i2])

    def hand(k, i1, i2):
        both = pl.ds(flat(i1, i2, 0), 2)
        push(own[k].at[both], other[k].at[both], pass_out.at[k], pass_in.at[k], partner)

    def step(mine, offset):
        return lax.rem(mine + offset + N, N)

    for m in range(2):
        for k, d, side in lanes:
            send3(k, d, side, m)
    for m in range(2):
        for k, d, side in lanes:
            send2(k, d, side, m, r[k])
    for k, d, side in lanes:
        await3(k, d, 0)
        send3(k, d, side, 2)
    for e, behind in enumerate(SIDES):
        for k in WEIGHTS:
            await3(k, e, 1)
        for m in range(2):
            for k, d, side in lanes:
                send2(k, d, side, m, step(r[k], -behind))
    for k, d, side in lanes:
        await3(k, d, 2)
    for m in range(2):
        for k, d, side in lanes:
            send2(k, d, side, m, step(r[k], 2))
    for m in range(2):
        for k, d, side in lanes:
            send1(k, d, side, m, q[k])
    for k in WEIGHTS:
        hand(k, p[k], q[k])

    for k in WEIGHTS:
        arrived(grad[k].at[1 - core], grad_in.at[k])
    for layer in range(2):
        for k in range(2):
            half = own[k].shape[-1]
            width = min(half, 1024)
            for h in range(2):

                @pl.loop(0, half // width)
                def _(c):
                    within = pl.ds(pl.multiple_of(c * width, width), width)
                    columns = pl.ds(pl.multiple_of(h * half + c * width, width), width)
                    total = grad[k][layer, h, :, within].astype(jnp.float32)
                    rows = total.shape[0] // 2
                    total = jnp.where(core == 0, total[:rows], total[rows:])
                    _, m, v = adamw(total, fresh[0][k][layer, :, columns], fresh[1][k][layer, :, columns], total)
                    fresh[0][k][layer, :, columns] = m
                    fresh[1][k][layer, :, columns] = v

        @pl.loop(0, own[2].shape[-2] // depth)
        def _(c):
            rows = pl.ds(pl.multiple_of(c * depth, depth), depth)
            total = grad[2][layer, core, rows].astype(jnp.float32)
            _, m, v = adamw(total, fresh[0][2][layer, rows], fresh[1][2][layer, rows], total)
            fresh[0][2][layer, rows] = m
            fresh[1][2][layer, rows] = v

    for offset in (0, -1, 1, 2):
        for k, d, side in lanes:
            await2(k, d, 0, step(r[k], offset))
            send2(k, d, side, 2, step(r[k], offset))
    for e, behind in enumerate(SIDES):
        for offset in (0, -1, 1, 2):
            for k in WEIGHTS:
                await2(k, e, 1, step(r[k], offset))
        for m in range(2):
            for k, d, side in lanes:
                send1(k, d, side, m, step(q[k], -behind))
        for k in WEIGHTS:
            hand(k, p[k], step(q[k], -behind))
    for offset in (0, -1, 1, 2):
        for k, d, side in lanes:
            await2(k, d, 2, step(r[k], offset))
    for m in range(2):
        for k, d, side in lanes:
            send1(k, d, side, m, step(q[k], 2))
    for k in WEIGHTS:
        hand(k, p[k], step(q[k], 2))
    for offset in (0, -1, 1, 2):
        for k, d, side in lanes:
            await1(k, d, 0, step(q[k], offset))
            send1(k, d, side, 2, step(q[k], offset))
    for offset in (0, -1, 1, 2):
        for k, d, side in lanes:
            await1(k, d, 1, step(q[k], offset))
            hand(k, step(p[k], -side), step(q[k], offset))
    for offset in (0, -1, 1, 2):
        for k in WEIGHTS:
            for d in range(2):
                await1(k, d, 2, step(q[k], offset))
            hand(k, step(p[k], 2), step(q[k], offset))

    for k in WEIGHTS:
        arrived(own[k], part_out.at[k])
        arrived(grad[k].at[0], grad_out.at[k])
        for i in range(2):
            arrived(theirs[i][k], theirs_out.at[i, k])
        for d in range(2):
            arrived(own[k].at[0:12], out1.at[k, d])
            arrived(own[k].at[0:3], out2.at[k, d])
            arrived(own[k].at[0, 0:3], out3.at[k, d])
        arrived(own[k], pass_out.at[k])
        arrived(other[k], pass_in.at[k])


def write_kernel(*refs):
    own, other, moments, out, written, sem, moment_sem = refs[0:3], refs[3:6], refs[6:12], refs[12:15], refs[15:21], refs[21], refs[22]
    _, core = place()
    copies = []
    for i1 in range(N):
        for i2 in range(N):
            for h in range(2):
                for k in WEIGHTS:
                    j = (i1 * N + i2) * 2 + h
                    copies.append(pltpu.make_async_copy(own[k].at[j], piece(out[k], k, core, i1, i2, h), sem.at[k, 0]))
                    copies.append(pltpu.make_async_copy(other[k].at[j], piece(out[k], k, 1 - core, i1, i2, h), sem.at[k, 1]))
    small = [pltpu.make_async_copy(a, b, moment_sem.at[i]) for i, (a, b) in enumerate(zip(moments, written, strict=True))]
    for copy in copies + small:
        copy.start()
    for k in WEIGHTS:
        pltpu.make_async_copy(own[k], own[k], sem.at[k, 0]).wait()
        pltpu.make_async_copy(other[k], other[k], sem.at[k, 1]).wait()
    for copy in small:
        copy.wait()


ANY = pl.BlockSpec(memory_space=pl.ANY)
VMEM = pl.BlockSpec(memory_space=pltpu.VMEM)
LIMIT = 6 * 2**20
SMALL = 2**20


def solution(mesh):
    bf16, f32, dma = jnp.bfloat16, jnp.float32, pltpu.SemaphoreType.DMA

    def step(*arrays):
        terms, weights, m, v = (arrays[i : i + 3] for i in (0, 3, 6, 9))
        views, blocks = [], []
        for k, w in enumerate(weights):
            layers, rows, columns = w.shape
            block = rows // N**3
            views.append((layers, N, N, N, block, columns) if k < 2 else (layers, N, N, N, 2, block // 2, columns))
            blocks.append((block, columns // 2) if k < 2 else (block // 2, columns))
        each = lambda *lead: [pltpu.VMEM((*lead, *b), bf16) for b in blocks]
        moment = [pltpu.VMEM(one.shape, f32) for one in (*m, *v)]
        layer = [pltpu.VMEM(one.shape[1:], f32) for one in (*m, *v)]
        results = pl.pallas_call(
            step_kernel,
            out_shape=[*each(2 * N * N, N), *each(2 * N * N, N), *moment],
            in_specs=[ANY] * 12,
            out_specs=[VMEM] * 12,
            scratch_shapes=[
                *each(2, 2, N), *each(2, 2), *(pltpu.VMEM(view[4:], bf16) for view in views),
                *layer,
                dma((3, 2 * N * N)), dma((3,)),
                dma((3, 2, 3, N)), dma((3, 2)),
                dma((3, 2, 3, N)), dma((3, 2)),
                dma((3, 2, 3)), dma((3, 2)),
                dma((3, 2, 2)),
                dma((3,)), dma((2, 3)), dma((2, 3)), dma((2, 3)), dma((3,)), dma((3,)),
                dma((3, 2, 3, N)), dma((3, 2)),
                dma((3, 2, 3, N)), dma((3, 2)),
                dma((3, 2, 3)), dma((3, 2)),
                dma((3,)), dma((3,)), pltpu.SemaphoreType.REGULAR,
            ],
            compiler_params=pltpu.CompilerParams(collective_id=0, has_side_effects=True, vmem_limit_bytes=LIMIT),
            name="step",
        )(*(t.reshape(view) for t, view in zip(terms, views, strict=True)), *(w.reshape(view) for w, view in zip(weights, views, strict=True)), *m, *v)
        out = pl.pallas_call(
            write_kernel,
            out_shape=[*(jax.ShapeDtypeStruct(view, bf16) for view in views), *(jax.ShapeDtypeStruct(one.shape, f32) for one in (*m, *v))],
            in_specs=[VMEM] * 12,
            out_specs=[ANY] * 9,
            scratch_shapes=[dma((3, 2)), dma((6,))],
            compiler_params=pltpu.CompilerParams(vmem_limit_bytes=SMALL),
            name="write",
        )(*results)
        return (*(w.reshape(old.shape) for w, old in zip(out[:3], weights, strict=True)), *out[3:])

    all_of, cut = P(None, None, None), P(None, "dp", None)
    return jax.shard_map(
        step,
        mesh=mesh,
        in_specs=(P(("rep", "dp"), None, None, None),) * 3 + (all_of,) * 3 + (cut,) * 6,
        out_specs=(P("rep", None, None),) * 3 + (P("rep", "dp", None),) * 6,
        check_vma=False,
    )
```

```python
import functools

import jax
import jax.numpy as jnp
from jax import lax
from jax.experimental import pallas as pl
from jax.experimental.pallas import tpu as pltpu
from jax.sharding import PartitionSpec as P

N = 4
MESH = pl.DeviceIdType.MESH
ORDER = ((0, 1, 2), (1, 2, 0), (2, 0, 1))
SIDES = (1, -1)
WEIGHTS = range(3)


def adamw(w, m, v, g):
    m = 0.9 * m + 0.1 * g
    v = 0.95 * v + 0.05 * g * g
    step = m * lax.rsqrt(v + 1e-8) + 0.1 * w
    return w - 0.02 * step, m, v


def place():
    me = lax.axis_index("dp")
    core = lax.rem(me, 2)
    chip = me // 2
    return (chip // (N * N), lax.rem(chip // N, N), lax.rem(chip, N)), core


def device(chip, core):
    return {"dp": ((chip[0] * N + chip[1]) * N + chip[2]) * 2 + core}


def neighbour(chip, core, axis, side):
    moved = list(chip)
    moved[axis] = lax.rem(chip[axis] + side + N, N)
    return device(moved, core)


def greet(chip, core):
    barrier = pltpu.get_barrier_semaphore()
    others = [device(chip, 1 - core)] + [neighbour(chip, core, axis, side) for axis in range(3) for side in SIDES]
    for other in others:
        pl.semaphore_signal(barrier, inc=1, device_id=other, device_id_type=MESH)
    pl.semaphore_wait(barrier, len(others))


def piece(ref, k, layer, i1, i2, h):
    if k == 2:
        return ref.at[layer, i2, :, i1, h]
    half = ref.shape[-1] // 2
    columns = pl.ds(pl.multiple_of(h * half, half), half)
    if k == 0:
        return ref.at[layer, i1, i2, :, :, columns]
    return ref.at[layer, :, i1, i2, :, columns]


def far(m):
    return (4 - m) // 2


def half_of(side, m):
    h = lax.rem(m, 2) * (1 - m // 2) if not isinstance(m, int) else (m % 2) * (1 - m // 2)
    return h if side == 1 else 1 - h


def target(mine, side, m):
    return lax.rem(mine + side * far(m) + N, N)


def turn(mine, s):
    return lax.rem(mine + 2 - s + (s // 2) * (2 * s - 1) + N, N)


def put_sum(out, sources):
    def one(out, sources):
        total = sources[0][...].astype(jnp.float32)
        for source in sources[1:]:
            total = total + source[...].astype(jnp.float32)
        out[...] = total.astype(out.dtype)

    if len(out.shape) == 2:
        one(out, sources)
    else:

        @pl.loop(0, out.shape[0])
        def _(i):
            one(out.at[i], [source.at[i] for source in sources])


def rows_of_both(core, mine, theirs):
    low, high = jnp.where(core == 0, mine, theirs), jnp.where(core == 0, theirs, mine)
    return jnp.concatenate([low, high], axis=0)


def step_kernel(*refs):
    g, w, moments = refs[0:3], refs[3:6], (refs[6:9], refs[9:12])
    own, other, fresh = refs[12:15], refs[15:18], (refs[18:21], refs[21:24])
    ahead, grad, weight = (refs[24 + 3 * i : 27 + 3 * i] for i in range(3))
    theirs = (refs[33:36], refs[36:39])
    part_in, part_out, rs1_in, rs1_out, rs2_in, rs2_out, rs3_in, rs3_out, ahead_in = refs[39:48]
    weight_in, fresh_in, theirs_in, theirs_out, grad_in, grad_out = refs[48:54]
    pass_in, pass_out, ready, first_in = refs[54:58]
    chip, core = place()
    partner = device(chip, 1 - core)
    at = [[chip[axis] for axis in ORDER[k]] for k in WEIGHTS]
    p, q, r = zip(*at, strict=True)
    lanes = [(k, d, side) for d, side in enumerate(SIDES) for k in WEIGHTS]

    def flat(i1, i2, h):
        return (i1 * N + i2) * 2 + h

    def arrived(ref, sem):
        pltpu.make_async_copy(ref, ref, sem).wait()

    def push(src, dst, out_sem, in_sem, where):
        pltpu.make_async_remote_copy(
            src_ref=src, dst_ref=dst, send_sem=out_sem, recv_sem=in_sem, device_id=where, device_id_type=MESH
        ).start()

    def send(k, axis, side, src, dst, out_sem, in_sem):
        push(src, dst, out_sem, in_sem, neighbour(chip, core, ORDER[k][axis], side))

    def r1(k, d, m, i2):
        return other[k].at[(d * 3 + m) * N + i2]

    def r2(k, d, m, i3):
        return other[k].at[24 + d * 3 + m, i3]

    def r3(k, d, m):
        return other[k].at[30 + d, m]

    def spot(k, side, t):
        m, s = t // N, lax.rem(t, N)
        return target(p[k], side, m), turn(q[k], s), half_of(side, m)

    def give(t, j):
        for k, d, side in lanes:
            i1, i2, h = spot(k, side, t)
            push(piece(g[k], k, 1 - core, i1, i2, h), own[k].at[flat(i1, i2, h)], part_out.at[k], part_in.at[k, d, j], partner)

    def fetch(t):
        for k, d, side in lanes:
            i1, i2, h = spot(k, side, t)
            slot = lax.rem(t, 2)
            yield pltpu.make_async_copy(piece(g[k], k, core, i1, i2, h), ahead[k].at[slot, d], ahead_in.at[k, slot, d])

    def all_arrived(sem, j, pieces):
        for k, d, side in lanes:
            arrived(own[k].at[0:4] if pieces else own[k].at[0], sem.at[k, d, j])

    small = [pltpu.make_async_copy(w[k].at[core, chip[0], chip[1], chip[2]], weight[k], weight_in.at[k]) for k in WEIGHTS]
    small += [pltpu.make_async_copy(moments[i][k], fresh[i][k], fresh_in.at[i, k]) for i in range(2) for k in WEIGHTS]
    for copy in fetch(0):
        copy.start()
    greet(chip, core)

    for i3 in range(N):
        for k, d, side in lanes:
            i1, i2, h = spot(k, side, 0)
            source = piece(g[k], k, 1 - core, i1, i2, h).at[i3]
            push(source, own[k].at[flat(i1, i2, h), i3], part_out.at[k], first_in.at[k, d, i3], partner)

    @pl.loop(1, N)
    def _(t):
        give(t, t - 1)

    for copy in small:
        copy.start()
    for i in range(2):
        for k in WEIGHTS:
            push(moments[i][k].at[1 - core], theirs[i][k], theirs_out.at[i, k], theirs_in.at[i, k], partner)

    def first(m):
        def body(t):
            give(t + N, m + 3)

            @pl.when(t + 1 < 3 * N)
            def _():
                for copy in fetch(t + 1):
                    copy.start()

            pending = None
            for (k, d, side), copy in zip(lanes, fetch(t), strict=True):
                i1, i2, h = spot(k, side, t)
                copy.wait()
                here = own[k].at[flat(i1, i2, h)]
                if m == 0:
                    arrived(here, part_in.at[k, d, t - 1])
                sources = [here, ahead[k].at[lax.rem(t, 2), d]]
                if m == 2:
                    sources.append(r1(k, d, 0, i2))
                put_sum(here, sources)
                if pending is not None:
                    pending()
                pending = functools.partial(send, k, 0, side, here, r1(k, d, m, i2), rs1_out.at[k, d], rs1_in.at[k, d, 2 + i2 if m == 2 else m])
            pending()

        return body

    give(N, 3)
    for copy in fetch(1):
        copy.start()
    pending = None
    copies = fetch(0)
    for i3 in range(N):
        for k, d, side in lanes:
            i1, i2, h = spot(k, side, 0)
            if i3 == 0:
                next(copies).wait()
            here = own[k].at[flat(i1, i2, h), i3]
            arrived(here, first_in.at[k, d, i3])
            put_sum(here, [here, ahead[k].at[0, d, i3]])
            if pending is not None:
                pending()
            pending = functools.partial(send, k, 0, side, here, r1(k, d, 0, i2).at[i3], rs1_out.at[k, d], rs1_in.at[k, d, 0])
    pending()
    pl.loop(1, N)(first(0))
    all_arrived(part_in, 3, True)
    pl.loop(N, 2 * N)(first(1))
    all_arrived(part_in, 4, True)
    all_arrived(rs1_in, 0, True)
    pl.loop(2 * N, 3 * N)(first(2))

    def fetch_kept(m):
        for k, d, side in lanes:
            i2, h = target(q[k], side, m), half_of(side, m)
            yield pltpu.make_async_copy(piece(g[k], k, core, p[k], i2, h), ahead[k].at[m % 2, d], ahead_in.at[k, m % 2, d])

    for copy in fetch_kept(0):
        copy.start()

    def settled(k, side, m):
        i2, h = target(q[k], side, m), half_of(side, m)
        arrived(r1(k, h, 2, i2), rs1_in.at[k, h, 2 + i2])

    def terms(k, i2, h, i3, kept):
        here = own[k].at[flat(p[k], i2, h), i3]
        return here, [here, kept.at[i3], r1(k, 0, 2 - h, i2).at[i3], r1(k, 1, 1 + h, i2).at[i3]]

    all_arrived(part_in, 5, True)
    all_arrived(rs1_in, 1, True)
    for m in range(3):
        if m == 2:
            all_arrived(rs2_in, 0, False)
        for (k, d, side), copy in zip(lanes, fetch_kept(m), strict=True):
            settled(k, side, m)
            copy.wait()
        for copy in fetch_kept(m + 1):
            copy.start()

        @pl.loop(0, N)
        def _(s):
            pending = None
            for k, d, side in lanes:
                i2, h, i3 = target(q[k], side, m), half_of(side, m), turn(r[k], s)
                here, sources = terms(k, i2, h, i3, ahead[k].at[m % 2, d])
                if m == 2:
                    sources.append(r2(k, d, 0, i3))
                put_sum(here, sources)
                if pending is not None:
                    pending()
                pending = functools.partial(send, k, 1, side, here, r2(k, d, m, i3), rs2_out.at[k, d], rs2_in.at[k, d, 2 + i3 if m == 2 else m])
            pending()

    for copy in small:
        copy.wait()
    for i in range(2):
        for k in WEIGHTS:
            arrived(theirs[i][k], theirs_in.at[i, k])
    for (k, d, side), copy in zip(lanes, fetch_kept(3), strict=True):
        settled(k, side, 3)
        copy.wait()
    all_arrived(rs2_in, 1, False)
    for m in range(4):
        pending = None
        for k, d, side in lanes:
            h, i3 = half_of(side, m), target(r[k], side, m)
            here, sources = terms(k, q[k], h, i3, ahead[k].at[1, h])
            for e, m2 in ((0, 2 - h), (1, 1 + h)):
                if m2 == 2:
                    arrived(r2(k, e, 2, i3), rs2_in.at[k, e, 2 + i3])
                sources.append(r2(k, e, m2, i3))
            if m == 2:
                arrived(r3(k, d, 0), rs3_in.at[k, d, 0])
                sources.append(r3(k, d, 0))
            if m == 3:
                for e, m3 in ((0, 2 - h), (1, 1 + h)):
                    arrived(r3(k, e, m3), rs3_in.at[k, e, m3])
                    sources.append(r3(k, e, m3))
                here = grad[k].at[core, h]
            put_sum(here, sources)
            if pending is not None:
                pending()
            pending = None
            if m < 3:
                pending = functools.partial(send, k, 2, side, here, r3(k, d, m), rs3_out.at[k, d], rs3_in.at[k, d, m])
        if pending is not None:
            pending()

    for k in WEIGHTS:
        for d in range(2):
            arrived(own[k].at[0:12], rs1_out.at[k, d])
            arrived(own[k].at[0:3], rs2_out.at[k, d])
            arrived(own[k].at[0, 0:3], rs3_out.at[k, d])
    for where in [partner] + [neighbour(chip, core, axis, side) for axis in range(3) for side in SIDES]:
        pl.semaphore_signal(ready, inc=1, device_id=where, device_id_type=MESH)

    for k in range(2):
        half = own[k].shape[-1]
        width = min(half, 1024)
        for h in range(2):
            block = own[k].at[flat(p[k], q[k], h), r[k]]

            @pl.loop(0, half // width)
            def _(c):
                within = pl.ds(pl.multiple_of(c * width, width), width)
                columns = pl.ds(pl.multiple_of(h * half + c * width, width), width)
                m, v = (rows_of_both(core, fresh[i][k][core, :, columns], theirs[i][k][:, columns]) for i in range(2))
                new, _, _ = adamw(weight[k][:, columns].astype(jnp.float32), m, v, grad[k][core, h, :, within].astype(jnp.float32))
                block[:, within] = new.astype(block.dtype)

    depth = min(own[2].shape[-2], 16)
    for h in range(2):
        block = own[2].at[flat(p[2], q[2], h), r[2]]

        @pl.loop(0, own[2].shape[-2] // depth)
        def _(c):
            rows = pl.ds(pl.multiple_of(c * depth, depth), depth)
            m, v = (jnp.where(core == h, fresh[i][2][core, rows], theirs[i][2][rows]) for i in range(2))
            new, _, _ = adamw(weight[2][h, rows].astype(jnp.float32), m, v, grad[2][core, h, rows].astype(jnp.float32))
            block[rows] = new.astype(block.dtype)

    for k in WEIGHTS:
        push(grad[k].at[core], grad[k].at[core], grad_out.at[k], grad_in.at[k], partner)
    pl.semaphore_wait(ready, 7)

    def source(mine, side, m):
        return mine if m < 2 else lax.rem(mine - side + N, N)

    def send3(k, d, side, m):
        i3, h = source(r[k], side, m), half_of(side, m)
        ref = own[k].at[flat(p[k], q[k], h), i3]
        send(k, 2, side, ref, ref, rs3_out.at[k, d], rs3_in.at[k, d, m])

    def send2(k, d, side, m, i3):
        i2, h = source(q[k], side, m), half_of(side, m)
        ref = own[k].at[flat(p[k], i2, h), i3]
        send(k, 1, side, ref, ref, rs2_out.at[k, d], rs2_in.at[k, d, (i3, 4, 5)[m]])

    def send1(k, d, side, m, i2):
        i1, h = source(p[k], side, m), half_of(side, m)
        ref = own[k].at[flat(i1, i2, h)]
        send(k, 0, side, ref, ref, rs1_out.at[k, d], rs1_in.at[k, d, (i2, 4, 5 + i2)[m]])

    def await3(k, d, m):
        arrived(own[k].at[0, 0], rs3_in.at[k, d, m])

    def await2(k, d, i3):
        arrived(own[k].at[0, 0], rs2_in.at[k, d, i3])

    def await1(k, d, m, i2):
        arrived(own[k].at[0], rs1_in.at[k, d, (i2, None, 5 + i2)[m]])

    def hand(k, i1, i2):
        both = pl.ds(flat(i1, i2, 0), 2)
        push(own[k].at[both], other[k].at[both], pass_out.at[k], pass_in.at[k], partner)

    def step(mine, offset):
        return lax.rem(mine + offset + N, N)

    for m in range(2):
        for k, d, side in lanes:
            send3(k, d, side, m)
    for m in range(2):
        for k, d, side in lanes:
            send2(k, d, side, m, r[k])
    for k, d, side in lanes:
        await3(k, d, 0)
        send3(k, d, side, 2)
    for e, behind in enumerate(SIDES):
        for k in WEIGHTS:
            await3(k, e, 1)
        for m in range(2):
            for k, d, side in lanes:
                send2(k, d, side, m, step(r[k], -behind))
    for k, d, side in lanes:
        await3(k, d, 2)
    for m in range(2):
        for k, d, side in lanes:
            send2(k, d, side, m, step(r[k], 2))
    for m in range(2):
        for k, d, side in lanes:
            send1(k, d, side, m, q[k])
    for k in WEIGHTS:
        hand(k, p[k], q[k])

    for k in WEIGHTS:
        arrived(grad[k].at[1 - core], grad_in.at[k])
    for layer in range(2):
        for k in range(2):
            half = own[k].shape[-1]
            width = min(half, 1024)
            for h in range(2):

                @pl.loop(0, half // width)
                def _(c):
                    within = pl.ds(pl.multiple_of(c * width, width), width)
                    columns = pl.ds(pl.multiple_of(h * half + c * width, width), width)
                    total = grad[k][layer, h, :, within].astype(jnp.float32)
                    rows = total.shape[0] // 2
                    total = jnp.where(core == 0, total[:rows], total[rows:])
                    _, m, v = adamw(total, fresh[0][k][layer, :, columns], fresh[1][k][layer, :, columns], total)
                    fresh[0][k][layer, :, columns] = m
                    fresh[1][k][layer, :, columns] = v

        @pl.loop(0, own[2].shape[-2] // depth)
        def _(c):
            rows = pl.ds(pl.multiple_of(c * depth, depth), depth)
            total = grad[2][layer, core, rows].astype(jnp.float32)
            _, m, v = adamw(total, fresh[0][2][layer, rows], fresh[1][2][layer, rows], total)
            fresh[0][2][layer, rows] = m
            fresh[1][2][layer, rows] = v

    for offset in (0, -1, 1, 2):
        for k, d, side in lanes:
            await2(k, d, step(r[k], offset))
            send2(k, d, side, 2, step(r[k], offset))
    for e, behind in enumerate(SIDES):
        for k in WEIGHTS:
            arrived(own[k].at[0], rs2_in.at[k, e, 4])
        for m in range(2):
            for k, d, side in lanes:
                send1(k, d, side, m, step(q[k], -behind))
        for k in WEIGHTS:
            hand(k, p[k], step(q[k], -behind))
    all_arrived(rs2_in, 5, False)
    for m in range(2):
        for k, d, side in lanes:
            send1(k, d, side, m, step(q[k], 2))
    for k in WEIGHTS:
        hand(k, p[k], step(q[k], 2))
    for offset in (0, -1, 1):
        for k, d, side in lanes:
            await1(k, d, 0, step(q[k], offset))
            send1(k, d, side, 2, step(q[k], offset))
    for k, d, side in lanes:
        await1(k, d, 0, step(q[k], 2))
    for i3 in range(N):
        for k, d, side in lanes:
            ref = own[k].at[flat(source(p[k], side, 2), step(q[k], 2), half_of(side, 2)), i3]
            send(k, 0, side, ref, ref, rs1_out.at[k, d], first_in.at[k, d, i3])
    all_arrived(rs1_in, 4, True)
    for offset in (0, -1, 1, 2):
        for k, d, side in lanes:
            hand(k, step(p[k], -side), step(q[k], offset))
    for offset in (0, -1, 1):
        for k in WEIGHTS:
            for d in range(2):
                await1(k, d, 2, step(q[k], offset))
            hand(k, step(p[k], 2), step(q[k], offset))
    for i3 in range(N):
        for k in WEIGHTS:
            for d in range(2):
                arrived(own[k].at[0, 0], first_in.at[k, d, i3])
            both = pl.ds(flat(step(p[k], 2), step(q[k], 2), 0), 2)
            push(own[k].at[both, i3], other[k].at[both, i3], pass_out.at[k], pass_in.at[k], partner)

    for k in WEIGHTS:
        arrived(own[k], part_out.at[k])
        arrived(grad[k].at[0], grad_out.at[k])
        for i in range(2):
            arrived(theirs[i][k], theirs_out.at[i, k])
        for d in range(2):
            arrived(own[k].at[0:12], rs1_out.at[k, d])
            arrived(own[k].at[0:3], rs2_out.at[k, d])
            arrived(own[k].at[0, 0:3], rs3_out.at[k, d])
        arrived(own[k], pass_out.at[k])
        arrived(other[k], pass_in.at[k])


def write_kernel(*refs):
    own, other, moments, out, written, sem, moment_sem = refs[0:3], refs[3:6], refs[6:12], refs[12:15], refs[15:21], refs[21], refs[22]
    _, core = place()
    copies = []
    for i1 in range(N):
        for i2 in range(N):
            for h in range(2):
                for k in WEIGHTS:
                    j = (i1 * N + i2) * 2 + h
                    copies.append(pltpu.make_async_copy(own[k].at[j], piece(out[k], k, core, i1, i2, h), sem.at[k, 0]))
                    copies.append(pltpu.make_async_copy(other[k].at[j], piece(out[k], k, 1 - core, i1, i2, h), sem.at[k, 1]))
    small = [pltpu.make_async_copy(a, b, moment_sem.at[i]) for i, (a, b) in enumerate(zip(moments, written, strict=True))]
    for copy in copies + small:
        copy.start()
    for k in WEIGHTS:
        pltpu.make_async_copy(own[k], own[k], sem.at[k, 0]).wait()
        pltpu.make_async_copy(other[k], other[k], sem.at[k, 1]).wait()
    for copy in small:
        copy.wait()


ANY = pl.BlockSpec(memory_space=pl.ANY)
VMEM = pl.BlockSpec(memory_space=pltpu.VMEM)
LIMIT = 6 * 2**20
SMALL = 2**20


def solution(mesh):
    bf16, f32, dma = jnp.bfloat16, jnp.float32, pltpu.SemaphoreType.DMA

    def step(*arrays):
        terms, weights, m, v = (arrays[i : i + 3] for i in (0, 3, 6, 9))
        views, blocks = [], []
        for k, w in enumerate(weights):
            layers, rows, columns = w.shape
            block = rows // N**3
            views.append((layers, N, N, N, block, columns) if k < 2 else (layers, N, N, N, 2, block // 2, columns))
            blocks.append((block, columns // 2) if k < 2 else (block // 2, columns))
        each = lambda *lead: [pltpu.VMEM((*lead, *b), bf16) for b in blocks]
        moment = [pltpu.VMEM(one.shape, f32) for one in (*m, *v)]
        layer = [pltpu.VMEM(one.shape[1:], f32) for one in (*m, *v)]
        results = pl.pallas_call(
            step_kernel,
            out_shape=[*each(2 * N * N, N), *each(2 * N * N, N), *moment],
            in_specs=[ANY] * 12,
            out_specs=[VMEM] * 12,
            scratch_shapes=[
                *each(2, 2, N), *each(2, 2), *(pltpu.VMEM(view[4:], bf16) for view in views),
                *layer,
                dma((3, 2, 6)), dma((3,)),
                dma((3, 2, 9)), dma((3, 2)),
                dma((3, 2, 6)), dma((3, 2)),
                dma((3, 2, 3)), dma((3, 2)),
                dma((3, 2, 2)),
                dma((3,)), dma((2, 3)), dma((2, 3)), dma((2, 3)), dma((3,)), dma((3,)),
                dma((3,)), dma((3,)), pltpu.SemaphoreType.REGULAR, dma((3, 2, N)),
            ],
            compiler_params=pltpu.CompilerParams(collective_id=0, has_side_effects=True, vmem_limit_bytes=LIMIT),
            name="step",
        )(*(t.reshape(view) for t, view in zip(terms, views, strict=True)), *(w.reshape(view) for w, view in zip(weights, views, strict=True)), *m, *v)
        out = pl.pallas_call(
            write_kernel,
            out_shape=[*(jax.ShapeDtypeStruct(view, bf16) for view in views), *(jax.ShapeDtypeStruct(one.shape, f32) for one in (*m, *v))],
            in_specs=[VMEM] * 12,
            out_specs=[ANY] * 9,
            scratch_shapes=[dma((3, 2)), dma((6,))],
            compiler_params=pltpu.CompilerParams(vmem_limit_bytes=SMALL),
            name="write",
        )(*results)
        return (*(w.reshape(old.shape) for w, old in zip(out[:3], weights, strict=True)), *out[3:])

    all_of, cut = P(None, None, None), P(None, "dp", None)
    return jax.shard_map(
        step,
        mesh=mesh,
        in_specs=(P(("rep", "dp"), None, None, None),) * 3 + (all_of,) * 3 + (cut,) * 6,
        out_specs=(P("rep", None, None),) * 3 + (P("rep", "dp", None),) * 6,
        check_vma=False,
    )
```

```python
import functools

import jax
import jax.numpy as jnp
from jax import lax
from jax.experimental import pallas as pl
from jax.experimental.pallas import tpu as pltpu
from jax.sharding import PartitionSpec as P

N = 4
MESH = pl.DeviceIdType.MESH
ORDER = ((0, 1, 2), (1, 2, 0), (2, 0, 1))
SIDES = (1, -1)
WEIGHTS = range(3)


def adamw(w, m, v, g):
    m = 0.9 * m + 0.1 * g
    v = 0.95 * v + 0.05 * g * g
    step = m * lax.rsqrt(v + 1e-8) + 0.1 * w
    return w - 0.02 * step, m, v


def place():
    me = lax.axis_index("dp")
    core = lax.rem(me, 2)
    chip = me // 2
    return (chip // (N * N), lax.rem(chip // N, N), lax.rem(chip, N)), core


def device(chip, core):
    return {"dp": ((chip[0] * N + chip[1]) * N + chip[2]) * 2 + core}


def neighbour(chip, core, axis, side):
    moved = list(chip)
    moved[axis] = lax.rem(chip[axis] + side + N, N)
    return device(moved, core)


def greet(chip, core):
    barrier = pltpu.get_barrier_semaphore()
    others = [device(chip, 1 - core)] + [neighbour(chip, core, axis, side) for axis in range(3) for side in SIDES]
    for other in others:
        pl.semaphore_signal(barrier, inc=1, device_id=other, device_id_type=MESH)
    pl.semaphore_wait(barrier, len(others))


def piece(ref, k, layer, i1, i2, h):
    if k == 2:
        return ref.at[layer, i2, :, i1, h]
    half = ref.shape[-1] // 2
    columns = pl.ds(pl.multiple_of(h * half, half), half)
    if k == 0:
        return ref.at[layer, i1, i2, :, :, columns]
    return ref.at[layer, :, i1, i2, :, columns]


def far(m):
    return (4 - m) // 2


def half_of(side, m):
    h = lax.rem(m, 2) * (1 - m // 2) if not isinstance(m, int) else (m % 2) * (1 - m // 2)
    return h if side == 1 else 1 - h


def target(mine, side, m):
    return lax.rem(mine + side * far(m) + N, N)


def turn(mine, s):
    return lax.rem(mine + 2 - s + (s // 2) * (2 * s - 1) + N, N)


def put_sum(out, sources):
    def one(out, sources):
        total = sources[0][...].astype(jnp.float32)
        for source in sources[1:]:
            total = total + source[...].astype(jnp.float32)
        out[...] = total.astype(out.dtype)

    if len(out.shape) == 2:
        one(out, sources)
    else:

        @pl.loop(0, out.shape[0])
        def _(i):
            one(out.at[i], [source.at[i] for source in sources])


def rows_of_both(core, mine, theirs):
    low, high = jnp.where(core == 0, mine, theirs), jnp.where(core == 0, theirs, mine)
    return jnp.concatenate([low, high], axis=0)


def step_kernel(*refs):
    g, w, moments = refs[0:3], refs[3:6], (refs[6:9], refs[9:12])
    own, other, fresh = refs[12:15], refs[15:18], (refs[18:21], refs[21:24])
    ahead, grad, weight = (refs[24 + 3 * i : 27 + 3 * i] for i in range(3))
    theirs = (refs[33:36], refs[36:39])
    part_in, part_out, rs1_in, rs1_out, rs2_in, rs2_out, rs3_in, rs3_out, ahead_in = refs[39:48]
    weight_in, fresh_in, theirs_in, theirs_out, grad_in, grad_out = refs[48:54]
    pass_in, pass_out, ready, first_in, lead_in, lead_out = refs[54:60]
    chip, core = place()
    partner = device(chip, 1 - core)
    at = [[chip[axis] for axis in ORDER[k]] for k in WEIGHTS]
    p, q, r = zip(*at, strict=True)
    lanes = [(k, d, side) for d, side in enumerate(SIDES) for k in WEIGHTS]

    def flat(i1, i2, h):
        return (i1 * N + i2) * 2 + h

    def arrived(ref, sem):
        pltpu.make_async_copy(ref, ref, sem).wait()

    def push(src, dst, out_sem, in_sem, where):
        pltpu.make_async_remote_copy(
            src_ref=src, dst_ref=dst, send_sem=out_sem, recv_sem=in_sem, device_id=where, device_id_type=MESH
        ).start()

    def send(k, axis, side, src, dst, out_sem, in_sem):
        push(src, dst, out_sem, in_sem, neighbour(chip, core, ORDER[k][axis], side))

    def r1(k, d, m, i2):
        return other[k].at[(d * 3 + m) * N + i2]

    def r2(k, d, m, i3):
        return other[k].at[24 + d * 3 + m, i3]

    def r3(k, d, m):
        return other[k].at[30 + d, m]

    def spot(k, side, t):
        m, s = t // N, lax.rem(t, N)
        return target(p[k], side, m), turn(q[k], s), half_of(side, m)

    def give(t):
        for k, d, side in lanes:
            i1, i2, h = spot(k, side, t)
            push(piece(g[k], k, 1 - core, i1, i2, h), own[k].at[flat(i1, i2, h)], part_out.at[k], part_in.at[k, flat(i1, i2, h)], partner)

    def fetch(t):
        for k, d, side in lanes:
            i1, i2, h = spot(k, side, t)
            slot = lax.rem(t, 2)
            yield pltpu.make_async_copy(piece(g[k], k, core, i1, i2, h), ahead[k].at[slot, d], ahead_in.at[k, slot, d])

    def part_arrived(k, i1, i2, h):
        arrived(own[k].at[flat(i1, i2, h)], part_in.at[k, flat(i1, i2, h)])

    small = [pltpu.make_async_copy(w[k].at[core, chip[0], chip[1], chip[2]], weight[k], weight_in.at[k]) for k in WEIGHTS]
    small += [pltpu.make_async_copy(moments[i][k], fresh[i][k], fresh_in.at[i, k]) for i in range(2) for k in WEIGHTS]
    leads = []
    for k, d, side in lanes:
        i1, i2, h = spot(k, side, 0)
        leads.append(pltpu.make_async_copy(piece(g[k], k, 1 - core, i1, i2, h), ahead[k].at[1, d], lead_in.at[k, d]))
    for copy in leads:
        copy.start()
    for copy in fetch(0):
        copy.start()
    greet(chip, core)

    for i3 in range(N):
        for (k, d, side), copy in zip(lanes, leads, strict=True):
            i1, i2, h = spot(k, side, 0)
            if i3 == 0:
                copy.wait()
            push(ahead[k].at[1, d, i3], own[k].at[flat(i1, i2, h), i3], lead_out.at[k], first_in.at[k, d, i3], partner)

    @pl.loop(1, N)
    def _(t):
        give(t)

    for copy in small:
        copy.start()
    for i in range(2):
        for k in WEIGHTS:
            push(moments[i][k].at[1 - core], theirs[i][k], theirs_out.at[i, k], theirs_in.at[i, k], partner)

    def first(last):
        def body(t):
            give(t + N)
            if last:

                @pl.when(t + 1 < 3 * N)
                def _():
                    for copy in fetch(t + 1):
                        copy.start()
            else:
                for copy in fetch(t + 1):
                    copy.start()
            pending = None
            for (k, d, side), copy in zip(lanes, fetch(t), strict=True):
                i1, i2, h = spot(k, side, t)
                copy.wait()
                part_arrived(k, i1, i2, h)
                here = own[k].at[flat(i1, i2, h)]
                sources = [here, ahead[k].at[lax.rem(t, 2), d]]
                if last:
                    arrived(r1(k, d, 0, i2), rs1_in.at[k, d, 0, i2])
                    sources.append(r1(k, d, 0, i2))
                put_sum(here, sources)
                if pending is not None:
                    pending()
                m = 2 if last else t // N
                pending = functools.partial(send, k, 0, side, here, r1(k, d, m, i2), rs1_out.at[k, d], rs1_in.at[k, d, m, i2])
            pending()

        return body

    give(N)
    pending = None
    copies = fetch(0)
    for i3 in range(N):
        for k, d, side in lanes:
            i1, i2, h = spot(k, side, 0)
            if i3 == 0:
                next(copies).wait()
            here = own[k].at[flat(i1, i2, h), i3]
            arrived(here, first_in.at[k, d, i3])
            put_sum(here, [here, ahead[k].at[0, d, i3]])
            if pending is not None:
                pending()
            pending = functools.partial(send, k, 0, side, here, r1(k, d, 0, i2).at[i3], rs1_out.at[k, d], rs1_in.at[k, d, 0, i2])
    pending()
    for k in WEIGHTS:
        arrived(own[k].at[0:2], lead_out.at[k])
    for copy in fetch(1):
        copy.start()
    pl.loop(1, 2 * N)(first(False))
    pl.loop(2 * N, 3 * N)(first(True))

    def fetch_kept(m):
        for k, d, side in lanes:
            i2, h = target(q[k], side, m), half_of(side, m)
            yield pltpu.make_async_copy(piece(g[k], k, core, p[k], i2, h), ahead[k].at[m % 2, d], ahead_in.at[k, m % 2, d])

    for copy in fetch_kept(0):
        copy.start()

    def settled(k, side, m):
        i2, h = target(q[k], side, m), half_of(side, m)
        part_arrived(k, p[k], i2, h)
        for d, m1 in ((0, 2 - h), (1, 1 + h)):
            arrived(r1(k, d, m1, i2), rs1_in.at[k, d, m1, i2])

    def terms(k, i2, h, i3, kept):
        here = own[k].at[flat(p[k], i2, h), i3]
        return here, [here, kept.at[i3], r1(k, 0, 2 - h, i2).at[i3], r1(k, 1, 1 + h, i2).at[i3]]

    for m in range(3):
        for (k, d, side), copy in zip(lanes, fetch_kept(m), strict=True):
            settled(k, side, m)
            copy.wait()
        for copy in fetch_kept(m + 1):
            copy.start()

        @pl.loop(0, N)
        def _(s):
            pending = None
            for k, d, side in lanes:
                i2, h, i3 = target(q[k], side, m), half_of(side, m), turn(r[k], s)
                here, sources = terms(k, i2, h, i3, ahead[k].at[m % 2, d])
                if m == 2:
                    arrived(r2(k, d, 0, i3), rs2_in.at[k, d, 0, i3])
                    sources.append(r2(k, d, 0, i3))
                put_sum(here, sources)
                if pending is not None:
                    pending()
                pending = functools.partial(send, k, 1, side, here, r2(k, d, m, i3), rs2_out.at[k, d], rs2_in.at[k, d, m, i3])
            pending()

    for copy in small:
        copy.wait()
    for i in range(2):
        for k in WEIGHTS:
            arrived(theirs[i][k], theirs_in.at[i, k])
    for (k, d, side), copy in zip(lanes, fetch_kept(3), strict=True):
        settled(k, side, 3)
        copy.wait()
    for m in range(4):
        pending = None
        for k, d, side in lanes:
            h, i3 = half_of(side, m), target(r[k], side, m)
            here, sources = terms(k, q[k], h, i3, ahead[k].at[1, h])
            for e, m2 in ((0, 2 - h), (1, 1 + h)):
                arrived(r2(k, e, m2, i3), rs2_in.at[k, e, m2, i3])
                sources.append(r2(k, e, m2, i3))
            if m == 2:
                arrived(r3(k, d, 0), rs3_in.at[k, d, 0])
                sources.append(r3(k, d, 0))
            if m == 3:
                for e, m3 in ((0, 2 - h), (1, 1 + h)):
                    arrived(r3(k, e, m3), rs3_in.at[k, e, m3])
                    sources.append(r3(k, e, m3))
                here = grad[k].at[core, h]
            put_sum(here, sources)
            if pending is not None:
                pending()
            pending = None
            if m < 3:
                pending = functools.partial(send, k, 2, side, here, r3(k, d, m), rs3_out.at[k, d], rs3_in.at[k, d, m])
        if pending is not None:
            pending()

    for k in WEIGHTS:
        for d in range(2):
            arrived(own[k].at[0:12], rs1_out.at[k, d])
            arrived(own[k].at[0:3], rs2_out.at[k, d])
            arrived(own[k].at[0, 0:3], rs3_out.at[k, d])
    for where in [partner] + [neighbour(chip, core, axis, side) for axis in range(3) for side in SIDES]:
        pl.semaphore_signal(ready, inc=1, device_id=where, device_id_type=MESH)

    for k in range(2):
        half = own[k].shape[-1]
        width = min(half, 1024)
        for h in range(2):
            block = own[k].at[flat(p[k], q[k], h), r[k]]

            @pl.loop(0, half // width)
            def _(c):
                within = pl.ds(pl.multiple_of(c * width, width), width)
                columns = pl.ds(pl.multiple_of(h * half + c * width, width), width)
                m, v = (rows_of_both(core, fresh[i][k][core, :, columns], theirs[i][k][:, columns]) for i in range(2))
                new, _, _ = adamw(weight[k][:, columns].astype(jnp.float32), m, v, grad[k][core, h, :, within].astype(jnp.float32))
                block[:, within] = new.astype(block.dtype)

    depth = min(own[2].shape[-2], 16)
    for h in range(2):
        block = own[2].at[flat(p[2], q[2], h), r[2]]

        @pl.loop(0, own[2].shape[-2] // depth)
        def _(c):
            rows = pl.ds(pl.multiple_of(c * depth, depth), depth)
            m, v = (jnp.where(core == h, fresh[i][2][core, rows], theirs[i][2][rows]) for i in range(2))
            new, _, _ = adamw(weight[2][h, rows].astype(jnp.float32), m, v, grad[2][core, h, rows].astype(jnp.float32))
            block[rows] = new.astype(block.dtype)

    for k in WEIGHTS:
        push(grad[k].at[core], grad[k].at[core], grad_out.at[k], grad_in.at[k], partner)
    pl.semaphore_wait(ready, 7)

    def source(mine, side, m):
        return mine if m < 2 else lax.rem(mine - side + N, N)

    def send3(k, d, side, m):
        i3, h = source(r[k], side, m), half_of(side, m)
        ref = own[k].at[flat(p[k], q[k], h), i3]
        send(k, 2, side, ref, ref, rs3_out.at[k, d], rs3_in.at[k, d, m])

    def send2(k, d, side, m, i3):
        i2, h = source(q[k], side, m), half_of(side, m)
        ref = own[k].at[flat(p[k], i2, h), i3]
        send(k, 1, side, ref, ref, rs2_out.at[k, d], rs2_in.at[k, d, m, i3])

    def send1(k, d, side, m, i2):
        i1, h = source(p[k], side, m), half_of(side, m)
        ref = own[k].at[flat(i1, i2, h)]
        send(k, 0, side, ref, ref, rs1_out.at[k, d], rs1_in.at[k, d, m, i2])

    def await3(k, d, m):
        arrived(own[k].at[0, 0], rs3_in.at[k, d, m])

    def await2(k, d, m, i3):
        arrived(own[k].at[0, 0], rs2_in.at[k, d, m, i3])

    def await1(k, d, m, i2):
        arrived(own[k].at[0], rs1_in.at[k, d, m, i2])

    def hand(k, i1, i2):
        both = pl.ds(flat(i1, i2, 0), 2)
        push(own[k].at[both], other[k].at[both], pass_out.at[k], pass_in.at[k], partner)

    def step(mine, offset):
        return lax.rem(mine + offset + N, N)

    for m in range(2):
        for k, d, side in lanes:
            send3(k, d, side, m)
    for m in range(2):
        for k, d, side in lanes:
            send2(k, d, side, m, r[k])
    for k, d, side in lanes:
        await3(k, d, 0)
        send3(k, d, side, 2)
    for e, behind in enumerate(SIDES):
        for k in WEIGHTS:
            await3(k, e, 1)
        for m in range(2):
            for k, d, side in lanes:
                send2(k, d, side, m, step(r[k], -behind))
    for k, d, side in lanes:
        await3(k, d, 2)
    for m in range(2):
        for k, d, side in lanes:
            send2(k, d, side, m, step(r[k], 2))
    for m in range(2):
        for k, d, side in lanes:
            send1(k, d, side, m, q[k])
    for k in WEIGHTS:
        hand(k, p[k], q[k])

    for k in WEIGHTS:
        arrived(grad[k].at[1 - core], grad_in.at[k])
    for layer in range(2):
        for k in range(2):
            half = own[k].shape[-1]
            width = min(half, 1024)
            for h in range(2):

                @pl.loop(0, half // width)
                def _(c):
                    within = pl.ds(pl.multiple_of(c * width, width), width)
                    columns = pl.ds(pl.multiple_of(h * half + c * width, width), width)
                    total = grad[k][layer, h, :, within].astype(jnp.float32)
                    rows = total.shape[0] // 2
                    total = jnp.where(core == 0, total[:rows], total[rows:])
                    _, m, v = adamw(total, fresh[0][k][layer, :, columns], fresh[1][k][layer, :, columns], total)
                    fresh[0][k][layer, :, columns] = m
                    fresh[1][k][layer, :, columns] = v

        @pl.loop(0, own[2].shape[-2] // depth)
        def _(c):
            rows = pl.ds(pl.multiple_of(c * depth, depth), depth)
            total = grad[2][layer, core, rows].astype(jnp.float32)
            _, m, v = adamw(total, fresh[0][2][layer, rows], fresh[1][2][layer, rows], total)
            fresh[0][2][layer, rows] = m
            fresh[1][2][layer, rows] = v

    for offset in (0, -1, 1, 2):
        for k, d, side in lanes:
            await2(k, d, 0, step(r[k], offset))
            send2(k, d, side, 2, step(r[k], offset))
    for e, behind in enumerate(SIDES):
        for offset in (0, -1, 1, 2):
            for k in WEIGHTS:
                await2(k, e, 1, step(r[k], offset))
        for m in range(2):
            for k, d, side in lanes:
                send1(k, d, side, m, step(q[k], -behind))
        for k in WEIGHTS:
            hand(k, p[k], step(q[k], -behind))
    for offset in (0, -1, 1, 2):
        for k, d, side in lanes:
            await2(k, d, 2, step(r[k], offset))
    for m in range(2):
        for k, d, side in lanes:
            send1(k, d, side, m, step(q[k], 2))
    for k in WEIGHTS:
        hand(k, p[k], step(q[k], 2))
    for offset in (0, -1, 1):
        for k, d, side in lanes:
            await1(k, d, 0, step(q[k], offset))
            send1(k, d, side, 2, step(q[k], offset))
    for k, d, side in lanes:
        await1(k, d, 0, step(q[k], 2))
    for i3 in range(N):
        for k, d, side in lanes:
            ref = own[k].at[flat(source(p[k], side, 2), step(q[k], 2), half_of(side, 2)), i3]
            send(k, 0, side, ref, ref, rs1_out.at[k, d], first_in.at[k, d, i3])
    for offset in (0, -1, 1, 2):
        for k, d, side in lanes:
            await1(k, d, 1, step(q[k], offset))
            hand(k, step(p[k], -side), step(q[k], offset))
    for offset in (0, -1, 1):
        for k in WEIGHTS:
            for d in range(2):
                await1(k, d, 2, step(q[k], offset))
            hand(k, step(p[k], 2), step(q[k], offset))
    for i3 in range(N):
        for k in WEIGHTS:
            for d in range(2):
                arrived(own[k].at[0, 0], first_in.at[k, d, i3])
            both = pl.ds(flat(step(p[k], 2), step(q[k], 2), 0), 2)
            push(own[k].at[both, i3], other[k].at[both, i3], pass_out.at[k], pass_in.at[k], partner)

    for k in WEIGHTS:
        arrived(own[k].at[0:30], part_out.at[k])
        arrived(grad[k].at[0], grad_out.at[k])
        for i in range(2):
            arrived(theirs[i][k], theirs_out.at[i, k])
        for d in range(2):
            arrived(own[k].at[0:12], rs1_out.at[k, d])
            arrived(own[k].at[0:3], rs2_out.at[k, d])
            arrived(own[k].at[0, 0:3], rs3_out.at[k, d])
        arrived(own[k], pass_out.at[k])
        arrived(other[k], pass_in.at[k])


def write_kernel(*refs):
    own, other, moments, out, written, sem, moment_sem = refs[0:3], refs[3:6], refs[6:12], refs[12:15], refs[15:21], refs[21], refs[22]
    _, core = place()
    copies = []
    for i1 in range(N):
        for i2 in range(N):
            for h in range(2):
                for k in WEIGHTS:
                    j = (i1 * N + i2) * 2 + h
                    copies.append(pltpu.make_async_copy(own[k].at[j], piece(out[k], k, core, i1, i2, h), sem.at[k, 0]))
                    copies.append(pltpu.make_async_copy(other[k].at[j], piece(out[k], k, 1 - core, i1, i2, h), sem.at[k, 1]))
    small = [pltpu.make_async_copy(a, b, moment_sem.at[i]) for i, (a, b) in enumerate(zip(moments, written, strict=True))]
    for copy in copies + small:
        copy.start()
    for k in WEIGHTS:
        pltpu.make_async_copy(own[k], own[k], sem.at[k, 0]).wait()
        pltpu.make_async_copy(other[k], other[k], sem.at[k, 1]).wait()
    for copy in small:
        copy.wait()


ANY = pl.BlockSpec(memory_space=pl.ANY)
VMEM = pl.BlockSpec(memory_space=pltpu.VMEM)
LIMIT = 6 * 2**20
SMALL = 2**20


def solution(mesh):
    bf16, f32, dma = jnp.bfloat16, jnp.float32, pltpu.SemaphoreType.DMA

    def step(*arrays):
        terms, weights, m, v = (arrays[i : i + 3] for i in (0, 3, 6, 9))
        views, blocks = [], []
        for k, w in enumerate(weights):
            layers, rows, columns = w.shape
            block = rows // N**3
            views.append((layers, N, N, N, block, columns) if k < 2 else (layers, N, N, N, 2, block // 2, columns))
            blocks.append((block, columns // 2) if k < 2 else (block // 2, columns))
        each = lambda *lead: [pltpu.VMEM((*lead, *b), bf16) for b in blocks]
        moment = [pltpu.VMEM(one.shape, f32) for one in (*m, *v)]
        layer = [pltpu.VMEM(one.shape[1:], f32) for one in (*m, *v)]
        results = pl.pallas_call(
            step_kernel,
            out_shape=[*each(2 * N * N, N), *each(2 * N * N, N), *moment],
            in_specs=[ANY] * 12,
            out_specs=[VMEM] * 12,
            scratch_shapes=[
                *each(2, 2, N), *each(2, 2), *(pltpu.VMEM(view[4:], bf16) for view in views),
                *layer,
                dma((3, 2 * N * N)), dma((3,)),
                dma((3, 2, 3, N)), dma((3, 2)),
                dma((3, 2, 3, N)), dma((3, 2)),
                dma((3, 2, 3)), dma((3, 2)),
                dma((3, 2, 2)),
                dma((3,)), dma((2, 3)), dma((2, 3)), dma((2, 3)), dma((3,)), dma((3,)),
                dma((3,)), dma((3,)), pltpu.SemaphoreType.REGULAR, dma((3, 2, N)), dma((3, 2)), dma((3,)),
            ],
            compiler_params=pltpu.CompilerParams(collective_id=0, has_side_effects=True, vmem_limit_bytes=LIMIT),
            name="step",
        )(*(t.reshape(view) for t, view in zip(terms, views, strict=True)), *(w.reshape(view) for w, view in zip(weights, views, strict=True)), *m, *v)
        out = pl.pallas_call(
            write_kernel,
            out_shape=[*(jax.ShapeDtypeStruct(view, bf16) for view in views), *(jax.ShapeDtypeStruct(one.shape, f32) for one in (*m, *v))],
            in_specs=[VMEM] * 12,
            out_specs=[ANY] * 9,
            scratch_shapes=[dma((3, 2)), dma((6,))],
            compiler_params=pltpu.CompilerParams(vmem_limit_bytes=SMALL),
            name="write",
        )(*results)
        return (*(w.reshape(old.shape) for w, old in zip(out[:3], weights, strict=True)), *out[3:])

    all_of, cut = P(None, None, None), P(None, "dp", None)
    return jax.shard_map(
        step,
        mesh=mesh,
        in_specs=(P(("rep", "dp"), None, None, None),) * 3 + (all_of,) * 3 + (cut,) * 6,
        out_specs=(P("rep", None, None),) * 3 + (P("rep", "dp", None),) * 6,
        check_vma=False,
    )
```
